256 devices in a mesh: dp: 16 (over y, x), rows: 16 (over z, core).
Axes of the slice: x: 4, y: 4, z: 8, core: 2. Of those that a mesh axis runs over, the one named last changes fastest.
Arguments:
- grad_out: bfloat16 [8192, 4096], P('dp', 'rows'), may hold values from -0.375 to 0.375
- activations: bfloat16 [8192, 4096], P('dp', 'rows'), may hold values from -6 to 6
- error_feedback: float32 [16, 4096, 4096], P('dp', 'rows'), may hold values from -6 to 6
- momentum: bfloat16 [4096, 4096], P('rows'), may hold values from -1.1953125 to 1.1953125
- right_factor: float32 [4096, 128], P('rows'), may hold values from -0.09375 to 0.09375
Outputs:
- new_error: float32 [16, 4096, 4096], P('dp', 'rows')
- new_momentum: bfloat16 [4096, 4096], P('rows')
- new_right: float32 [4096, 128], P('rows')
The draws below stay inside these ranges and needn't reach their ends.
All inputs are finite; a program needn't handle non-finite values.
Results may differ from the reference program's by a relative error of at most 0.0012.
Values may be sent and summed in bfloat16 or wider, within the bound.
A program may use at most 64 MiB of HBM per device.

```python
import jax
import jax.numpy as jnp
from jax import lax

OUTPUTS = 4096
INPUTS = 4096
FACTOR_RANK = 128
PASSES = 2
TOK_DEV = 512
TOKENS = 8192
REPLICAS = 16
N_DP = 16


def shard_levels(own_key, shape, split, low, top_value):
    factor_of, own = 1.0, jax.random.fold_in(own_key, 6)
    for position, blocks in split:
        steps = jnp.exp(jax.random.uniform(jax.random.fold_in(own, position), (blocks,), jnp.float32, low / len(split), top_value / len(split)))
        factor_of = factor_of * jnp.repeat(steps, shape[position] // blocks).reshape([-1 if axis == position else 1 for axis in range(len(shape))])
    return factor_of


def centred(rng, extent, spread, limit, shards=(), kind=jnp.bfloat16):
    values = spread * jax.random.normal(rng, extent, jnp.float32)
    if shards:
        values = values * shard_levels(rng, extent, shards, -0.22, 0.18)
    return jnp.clip(values, -limit, limit).astype(kind)


def setup_inputs(seed: int = 0) -> dict:
    seeds = jax.random.split(jax.random.key(seed), 6)
    grad_out = centred(seeds[0], (TOKENS, OUTPUTS), 0.0625, 0.375, ((0, 16), (1, 16)))
    activations = centred(seeds[1], (TOKENS, INPUTS), 1.0, 6.0, ((0, 16), (1, 16)))
    error_feedback = centred(seeds[2], (REPLICAS, OUTPUTS, INPUTS), 1.0, 6.0, ((0, 16), (1, 16)), jnp.float32)
    momentum = centred(seeds[3], (OUTPUTS, INPUTS), 0.2, 1.1953125, ((0, 16),))
    right_factor = centred(seeds[4], (INPUTS, FACTOR_RANK), INPUTS ** -0.5, 0.09375, ((0, 16),), jnp.float32)
    return dict(grad_out=grad_out, activations=activations, error_feedback=error_feedback, momentum=momentum, right_factor=right_factor)


MOMENTUM_RATE = 0.9
HIGHEST = lax.Precision.HIGHEST

def orthonormal(factor):
    gram_matrix = jnp.dot(factor.T.astype(jnp.float32), factor.astype(jnp.float32), precision=HIGHEST, preferred_element_type=jnp.float32)
    cholesky_lower = jnp.linalg.cholesky(gram_matrix)
    return jax.scipy.linalg.solve_triangular(cholesky_lower, factor.T, lower=True).T

def reference(grad_out, activations, error_feedback, momentum, right_factor):
    outs_grad = grad_out.astype(jnp.float32).reshape(N_DP, TOK_DEV, OUTPUTS)
    inputs_act = activations.astype(jnp.float32).reshape(N_DP, TOK_DEV, INPUTS)
    merged = jnp.einsum('rto,rti->roi', outs_grad, inputs_act, precision=HIGHEST) + error_feedback
    mean_grad = jnp.mean(merged, axis=0)
    right_full = right_factor
    left_factor = None
    for pass_index in range(PASSES):
        left_factor = jnp.dot(mean_grad.astype(jnp.float32), right_full.astype(jnp.float32), precision=HIGHEST, preferred_element_type=jnp.float32)
        left_factor = orthonormal(left_factor)
        right_full = jnp.dot(mean_grad.T.astype(jnp.float32), left_factor.astype(jnp.float32), precision=HIGHEST, preferred_element_type=jnp.float32)
    approx = jnp.dot(left_factor.astype(jnp.float32), right_full.T.astype(jnp.float32), precision=HIGHEST, preferred_element_type=jnp.float32)
    new_error = merged - approx[None]
    new_momentum = (MOMENTUM_RATE * momentum.astype(jnp.float32) + approx).astype(jnp.bfloat16)
    return (new_error, new_momentum, right_full)
```

```python
import functools

import jax
import jax.numpy as jnp
from jax import lax
from jax.experimental import pallas as pl
from jax.experimental.pallas import tpu as pltpu
from jax.sharding import PartitionSpec as P

MOMENTUM_RATE = 0.9
HIGHEST = lax.Precision.HIGHEST
MESH = pl.DeviceIdType.MESH
F32 = jnp.float32
PANEL = 16


def dot32(a, b, dims=((1,), (0,))):
    return lax.dot_general(
        a, b, (dims, ((), ())), precision=HIGHEST, preferred_element_type=F32
    )


def ring_dist(delta, size):
    return min(delta, size - delta)


def far_first(n_a, n_b, weight):
    pairs = [(a, b) for a in range(n_a) for b in range(n_b) if a or b]
    return sorted(pairs, key=lambda p: -weight(*p))


def cholesky_panels(aug, first, last):
    k = aug.shape[0]

    def panel(p, carry):
        base = pl.multiple_of(p * PANEL, PANEL)
        rows = aug[pl.ds(base, PANEL), :]
        lane = lax.broadcasted_iota(jnp.int32, (PANEL, 2 * k), 1)
        sub = lax.broadcasted_iota(jnp.int32, (PANEL, 1), 0)
        left = rows[:, :k]
        lane_k = lax.broadcasted_iota(jnp.int32, (PANEL, k), 1)
        cols = [
            jnp.sum(jnp.where(lane_k == base + i, left, 0.0), axis=1, keepdims=True)
            for i in range(PANEL)
        ]
        for i in range(PANEL):
            scale = lax.rsqrt(cols[i][i : i + 1, :])
            factor = jnp.where(sub > i, cols[i] * scale, 0.0)
            keep = sub == i
            head = rows[i : i + 1, :] * scale
            rows = jnp.where(keep, head, rows - factor * head)
            for m in range(i + 1, PANEL):
                cols[m] = cols[m] - factor * (cols[m][i : i + 1, :] * scale)
        aug[pl.ds(base, PANEL), :] = rows
        upper = jnp.where(lane_k >= base + PANEL, rows[:, :k], 0.0)
        aug[...] = aug[...] - dot32(upper.T, rows)
        return carry

    lax.fori_loop(first, last, panel, 0)


def body(
    nx, ny, nz, scale,
    grad, act, err, right0,
    merged_out, lhat_out, s_out, sown_out, inv_out,
    act_all, grad_t, err_v, merged, rb, m_tile, m_t,
    xr, yr, xs, ys, xf, yf, top, bottom,
    p_plane, r_plane, f_plane, p_col, r_col, f_col, aug, s_full,
    local_sem, up_send, up_recv, down_send, down_recv, sib_send, sib_recv,
    rb_send, rb_recv, x_send, x_recv, y_send, y_recv, xf_send, xf_recv, yf_send, yf_recv,
    ps_send, ps_recv, pg_send, pg_recv, cs_send, cs_recv, cg_send, cg_recv,
    ag_send, ag_recv, dd_send, dd_recv,
):
    d, j = lax.axis_index("dp"), lax.axis_index("rows")
    y, x = d // nx, d % nx
    z, c = j // 2, j % 2
    tok, cb = act.shape
    rb_rows = grad.shape[1]
    half_rows = rb_rows // 2
    n = nx * ny
    far = nz // 2
    th = tok // 2

    def plane_id(dy, dx):
        return (((y + dy) % ny) * nx + (x + dx) % nx, j)

    def col_id(dz, dc):
        return (d, ((z + dz) % nz) * 2 + (c + dc) % 2)

    plane = far_first(ny, nx, lambda a, b: ring_dist(a, ny) + ring_dist(b, nx))
    column = far_first(nz, 2, lambda a, b: ring_dist(a, nz) + 0.1 * b)

    def remote(src, dst, send, recv, device):
        return pltpu.make_async_remote_copy(
            src_ref=src, dst_ref=dst, send_sem=send, recv_sem=recv,
            device_id=device, device_id_type=MESH,
        )

    load_act = pltpu.make_async_copy(act, act_all.at[0, 0], local_sem.at[0])
    load_act.start()
    load_err = pltpu.make_async_copy(err.at[0], err_v, local_sem.at[1])
    load_err.start()

    barrier = pltpu.get_barrier_semaphore()
    for dy, dx in plane:
        pl.semaphore_signal(barrier, inc=1, device_id=plane_id(dy, dx), device_id_type=MESH)
    for dz, dc in column:
        pl.semaphore_signal(barrier, inc=1, device_id=col_id(dz, dc), device_id_type=MESH)
    grad_t[...] = grad[...].astype(F32).T.astype(jnp.bfloat16)
    load_act.wait()
    pl.semaphore_wait(barrier, len(plane) + len(column))

    def half(slot, h):
        return act_all.at[slot, 0, pl.ds(h * th, th)]

    def up(s, h):
        return remote(half((nz - s + 1) % nz, h), half(nz - s, h), up_send.at[s - 1, h], up_recv.at[s - 1, h], col_id(1, 0))

    def down(s, h):
        return remote(half(s - 1, h), half(s, h), down_send.at[s - 1, h], down_recv.at[s - 1, h], col_id(nz - 1, 0))

    def sibling(slot, h):
        return remote(half(slot, h), act_all.at[slot, 1, pl.ds(h * th, th)], sib_send.at[slot, h], sib_recv.at[slot, h], col_id(0, 1))

    up_list = [(s, h) for s in range(1, far) for h in (0, 1)] + [(far, 0)]
    down_list = [(s, h) for s in range(1, far) for h in (1, 0)] + [(far, 1)]

    for ua, da in zip(up_list[:2], down_list[:2]):
        if ua[0] == 1:
            up(*ua).start()
        if da[0] == 1:
            down(*da).start()
    for h in (0, 1):
        sibling(0, h).start()

    own_block = x * ny + y
    src_z, src_c = own_block // 2, own_block % 2
    rb_up = remote(rb, rb, rb_send.at[0], rb_recv, col_id(1, 0))
    rb_down = remote(rb, rb, rb_send.at[1], rb_recv, col_id(nz - 1, 0))
    rb_sib = remote(rb, rb, rb_send.at[2], rb_recv, col_id(0, 1))

    @pl.when(jnp.logical_and(z == src_z, c == src_c))
    def _():
        own = pltpu.make_async_copy(right0, rb, local_sem.at[2])
        own.start()
        own.wait()
        rb_up.start()
        if far > 1:
            rb_down.start()
        rb_sib.start()

    def relay_rb(s, upward):
        at = (z - s) if upward else (z + s)

        @pl.when(jnp.logical_and((at + nz) % nz == src_z, c == src_c))
        def _():
            rb_up.wait_recv()
            if upward and s < far:
                rb_up.start()
            if not upward and s < far - 1:
                rb_down.start()
            rb_sib.start()

    load_err.wait()
    def block_of(slot, dc):
        return ((z + slot) % nz) * 2 + (c + dc) % 2

    def columns(b):
        return pl.ds(pl.multiple_of(b * cb, cb), cb)

    def x_copy(b, dx):
        return remote(merged.at[pl.ds(0, half_rows), columns(b)], xr.at[b % ny, dx - 1],
                      x_send.at[b], x_recv.at[b % ny, dx - 1], plane_id(0, dx))

    def y_copy(b, dy):
        return remote(merged.at[pl.ds(half_rows, half_rows), columns(b)], yr.at[b // ny, dy - 1],
                      y_send.at[b], y_recv.at[b // ny, dy - 1], plane_id(dy, 0))

    def produce(slot, dc):
        if dc == 1:
            hs = (0, 1)
            for h in hs:
                sibling(slot, h).wait_recv()
        b = block_of(slot, dc)
        cols = columns(b)
        tile = jnp.dot(grad_t[...], act_all[slot, dc], preferred_element_type=F32)
        merged[:, cols] = tile + err_v[:, cols]
        owner_x, owner_y = b // ny, b % ny
        for dx in range(1, nx):
            @pl.when((owner_x - x + nx) % nx == dx)
            def _(dx=dx):
                x_copy(b, dx).start()
        for dy in range(1, ny):
            @pl.when((owner_y - y + ny) % ny == dy)
            def _(dy=dy):
                y_copy(b, dy).start()

    def xf_copy(dy):
        return remote(xs.at[dy - 1], xf.at[dy - 1], xf_send.at[dy - 1], xf_recv.at[dy - 1], plane_id(dy, 0))

    def yf_copy(dx):
        return remote(ys.at[dx - 1], yf.at[dx - 1], yf_send.at[dx - 1], yf_recv.at[dx - 1], plane_id(0, dx))

    def consume(slot, dc):
        b = block_of(slot, dc)
        cols = columns(b)
        owner_x, owner_y = b // ny, b % ny

        @pl.when(owner_x == x)
        def _():
            total = merged[pl.ds(0, half_rows), cols]
            for dx in range(1, nx):
                x_copy(b, dx).wait_recv()
                total = total + xr[b % ny, dx - 1]

            @pl.when(owner_y == y)
            def _():
                top[...] = total
            for dy in range(1, ny):
                @pl.when((owner_y - y + ny) % ny == dy)
                def _(dy=dy):
                    xs[dy - 1] = total
                    xf_copy(dy).start()

        @pl.when(owner_y == y)
        def _():
            total = merged[pl.ds(half_rows, half_rows), cols]
            for dy in range(1, ny):
                y_copy(b, dy).wait_recv()
                total = total + yr[b // ny, dy - 1]

            @pl.when(owner_x == x)
            def _():
                bottom[...] = total
            for dx in range(1, nx):
                @pl.when((owner_x - x + nx) % nx == dx)
                def _(dx=dx):
                    ys[dx - 1] = total
                    yf_copy(dx).start()

    produce(0, 0)
    later = {i: [] for i in range(nz + 3)}
    later[0].append((0, 1))
    for i, ((s, h), (t, g)) in enumerate(zip(up_list, down_list)):
        if s < far and h == 1:
            later[i] += [(nz - s, 0), (s, 0)]
            later[i + 1] += [(nz - s, 1), (s, 1)]
        if s == far:
            later[i] += [(far, 0)]
            later[i + 1] += [(far, 1)]
    done = [(0, 0)]
    steps = len(up_list)
    for i in range(steps + 1):
        if i < steps:
            (s, h), (t, g) = up_list[i], down_list[i]
            up(s, h).wait_recv()
            if s + 1 < far or (s + 1 == far and h == 0):
                up(s + 1, h).start()
            sibling(nz - s, h).start()
            down(t, g).wait_recv()
            if t + 1 < far or (t + 1 == far and g == 1):
                down(t + 1, g).start()
            sibling(t, g).start()
            if s == far or h == 1:
                relay_rb(s, True)
                if s < far:
                    relay_rb(s, False)
        fresh = later[i]
        for slot, dc in fresh:
            produce(slot, dc)
        for slot, dc in done:
            consume(slot, dc)
        done = list(fresh)
    for slot, dc in done:
        consume(slot, dc)

    store_merged = pltpu.make_async_copy(merged, merged_out, local_sem.at[1])
    store_merged.start()

    @pl.when(c != src_c)
    def _():
        rb_sib.wait_recv()

    acc = top[...]
    for dy in range(1, ny):
        xf_copy(dy).wait_recv()
        acc = acc + xf[dy - 1]
    m_tile[pl.ds(0, half_rows), :] = acc * scale
    acc = bottom[...]
    for dx in range(1, nx):
        yf_copy(dx).wait_recv()
        acc = acc + yf[dx - 1]
    m_tile[pl.ds(half_rows, half_rows), :] = acc * scale

    sr = rb_rows // n
    gr = aug.shape[0] // n
    k = aug.shape[0]

    def wait_bytes(ref, sem):
        pltpu.make_async_copy(ref, ref, sem).wait()

    def plane_scatter(stage):
        for i, (dy, dx) in enumerate(plane):
            dev = plane_id(dy, dx)
            remote(p_plane.at[stage, dev[0]], r_plane.at[stage, i], ps_send.at[stage], ps_recv.at[stage], dev).start()

    def plane_gather(stage):
        wait_bytes(r_plane.at[stage], ps_recv.at[stage])
        total = p_plane[stage, d]
        for i in range(len(plane)):
            total = total + r_plane[stage, i]
        f_plane[stage, d] = total
        for dy, dx in plane:
            remote(f_plane.at[stage, d], f_plane.at[stage, d], pg_send.at[stage], pg_recv.at[stage], plane_id(dy, dx)).start()

    def plane_finish(stage):
        wait_bytes(r_plane.at[stage], pg_recv.at[stage])
        return f_plane[stage].reshape(rb_rows, k)

    def col_scatter(stage):
        for i, (dz, dc) in enumerate(column):
            dev = col_id(dz, dc)
            remote(p_col.at[stage, dev[1]], r_col.at[stage, i], cs_send.at[stage], cs_recv.at[stage], dev).start()

    def col_gather(stage):
        wait_bytes(r_col.at[stage], cs_recv.at[stage])
        total = p_col[stage, j]
        for i in range(len(column)):
            total = total + r_col[stage, i]
        f_col[stage, j] = total
        for dz, dc in column:
            remote(f_col.at[stage, j], f_col.at[stage, j], cg_send.at[stage], cg_recv.at[stage], col_id(dz, dc)).start()

    def col_finish(stage):
        wait_bytes(r_col.at[stage], cg_recv.at[stage])
        both = f_col[stage]
        return both[:, :sr].reshape(cb, k), both[:, sr:].reshape(k, k)

    def set_aug(gram):
        row = lax.broadcasted_iota(jnp.int32, (k, k), 0)
        col = lax.broadcasted_iota(jnp.int32, (k, k), 1)
        aug[:, :k] = gram
        aug[:, k:] = jnp.where(row == col, 1.0, 0.0).astype(F32)

    panels = k // PANEL

    p_plane[0] = dot32(m_tile[...], rb[...]).reshape(n, sr, k)
    plane_scatter(0)
    m_t[...] = m_tile[...].T
    plane_gather(0)
    left = plane_finish(0)
    p_col[0, :, :sr] = dot32(m_t[...], left).reshape(n, sr, k)
    p_col[0, :, sr:] = dot32(left, left, ((0,), (0,))).reshape(n, gr, k)
    col_scatter(0)
    col_gather(0)
    s_one, gram_one = col_finish(0)
    p_plane[1] = dot32(m_tile[...], s_one).reshape(n, sr, k)
    plane_scatter(1)
    set_aug(gram_one)
    cholesky_panels(aug, 0, panels // 2)
    plane_gather(1)
    cholesky_panels(aug, panels // 2, panels)
    left = dot32(plane_finish(1), aug[:, k:], ((1,), (1,)))
    p_col[1, :, :sr] = dot32(m_t[...], left).reshape(n, sr, k)
    p_col[1, :, sr:] = dot32(left, left, ((0,), (0,))).reshape(n, gr, k)
    col_scatter(1)
    col_gather(1)
    _, gram_two = col_finish(1)

    hc = cb // 2
    own_half = f_col[1, pl.ds(c * (n // 2), n // 2), :sr, :].reshape(hc, k)
    s_full[x, y, pl.ds(pl.multiple_of(c * hc, hc), hc), :] = own_half
    q = hc // 2
    q0 = pl.ds(pl.multiple_of(c * hc, hc), q)
    q1 = pl.ds(pl.multiple_of(c * hc + q, q), q)

    def ag1x(dx):
        ref = s_full.at[x, y, q0]
        return remote(ref, ref, ag_send.at[0, dx - 1], ag_recv.at[0, dx - 1], plane_id(0, dx))

    def ag1y(dy):
        ref = s_full.at[x, y, q1]
        return remote(ref, ref, ag_send.at[1, dy - 1], ag_recv.at[1, dy - 1], plane_id(dy, 0))

    def ag2x(dy):
        ref = s_full.at[:, y, q0]
        return remote(ref, ref, ag_send.at[2, dy - 1], ag_recv.at[2, dy - 1], plane_id(dy, 0))

    def ag2y(dx):
        ref = s_full.at[x, :, q1]
        return remote(ref, ref, ag_send.at[3, dx - 1], ag_recv.at[3, dx - 1], plane_id(0, dx))

    def d2d(i, where):
        ref = s_full.at[where]
        return remote(ref, ref, dd_send.at[i], dd_recv.at[i], col_id(0, 1))

    for dx in range(1, nx):
        ag1x(dx).start()
    for dy in range(1, ny):
        ag1y(dy).start()
    set_aug(gram_two)
    cholesky_panels(aug, 0, panels // 2)
    for dx in range(1, nx):
        ag1x(dx).wait_recv()
    for dy in range(1, ny):
        ag2x(dy).start()
    for dy in range(1, ny):
        ag1y(dy).wait_recv()
    for dx in range(1, nx):
        ag2y(dx).start()
    cholesky_panels(aug, panels // 2, panels)
    inverse = aug[:, k:]
    inv_out[...] = inverse
    lhat_out[...] = dot32(dot32(left, inverse, ((1,), (1,))), inverse)

    for dy in range(1, ny):
        ag2x(dy).wait_recv()
    for dx in range(1, nx):
        ag2y(dx).wait_recv()
    share = d2d(0, (slice(None), slice(None), pl.ds(pl.multiple_of(c * hc, hc), hc)))
    share.start()
    share.wait_recv()
    store_s = pltpu.make_async_copy(s_full, s_out, local_sem.at[0])
    store_s.start()
    sown_out[...] = s_full[j // ny, j % ny]

    for s, h in up_list:
        up(s, h).wait_send()
    for s, h in down_list:
        down(s, h).wait_send()
    for slot in range(nz):
        for h in (0, 1):
            sibling(slot, h).wait_send()
    is_src_core = c == src_c
    away = (z - src_z + nz) % nz

    @pl.when(jnp.logical_and(is_src_core, away < far))
    def _():
        rb_up.wait_send()
    if far > 1:
        @pl.when(jnp.logical_and(is_src_core, jnp.logical_or(away == 0, away > far + 1)))
        def _():
            rb_down.wait_send()

    @pl.when(is_src_core)
    def _():
        rb_sib.wait_send()
    for b in range(n):
        if nx > 1:
            @pl.when(b // ny != x)
            def _(b=b):
                x_copy(b, 1).wait_send()
        if ny > 1:
            @pl.when(b % ny != y)
            def _(b=b):
                y_copy(b, 1).wait_send()
    for dy in range(1, ny):
        xf_copy(dy).wait_send()
        ag1y(dy).wait_send()
        ag2x(dy).wait_send()
    for dx in range(1, nx):
        yf_copy(dx).wait_send()
        ag1x(dx).wait_send()
        ag2y(dx).wait_send()
    for stage in (0, 1):
        wait_bytes(r_plane.at[stage], ps_send.at[stage])
        wait_bytes(r_plane.at[stage], pg_send.at[stage])
        wait_bytes(r_col.at[stage], cs_send.at[stage])
        wait_bytes(r_col.at[stage], cg_send.at[stage])
    share.wait_send()
    store_merged.wait()
    store_s.wait()


def finish_body(merged, lhat, s, momentum, sown, inverse, error, new_momentum, right):
    approx = dot32(lhat[...], s[...], ((1,), (1,)))
    error[0] = merged[...] - approx
    new_momentum[...] = (MOMENTUM_RATE * momentum[...].astype(F32) + approx).astype(jnp.bfloat16)

    @pl.when(pl.program_id(0) == 0)
    def _():
        right[...] = dot32(sown[...], inverse[...], ((1,), (1,)))


def per_device(nx, ny, nz, grad_out, activations, error_feedback, momentum, right_factor):
    n = nx * ny
    tok, cb = activations.shape
    rows = grad_out.shape[1]
    total = error_feedback.shape[2]
    k = right_factor.shape[1]
    sr, gr, hr = rows // n, k // n, rows // 2
    far = nz // 2
    vmem, dma = pltpu.VMEM, pltpu.SemaphoreType.DMA
    scratch = [
        vmem((nz, 2, tok, cb), jnp.bfloat16),
        vmem((rows, tok), jnp.bfloat16),
        vmem((rows, total), F32),
        vmem((rows, total), F32),
        vmem((cb, k), F32),
        vmem((rows, cb), F32),
        vmem((cb, rows), F32),
        vmem((ny, max(nx - 1, 1), hr, cb), F32),
        vmem((nx, max(ny - 1, 1), hr, cb), F32),
        vmem((max(ny - 1, 1), hr, cb), F32),
        vmem((max(nx - 1, 1), hr, cb), F32),
        vmem((max(ny - 1, 1), hr, cb), F32),
        vmem((max(nx - 1, 1), hr, cb), F32),
        vmem((hr, cb), F32),
        vmem((hr, cb), F32),
        vmem((2, n, sr, k), F32),
        vmem((2, n - 1, sr, k), F32),
        vmem((2, n, sr, k), F32),
        vmem((2, n, sr + gr, k), F32),
        vmem((2, n - 1, sr + gr, k), F32),
        vmem((2, n, sr + gr, k), F32),
        vmem((k, 2 * k), F32),
        vmem((nx, ny, cb, k), F32),
        dma((3,)),
        dma((far, 2)), dma((far, 2)), dma((far, 2)), dma((far, 2)),
        dma((nz, 2)), dma((nz, 2)),
        dma((3,)), dma,
        dma((n,)), dma((ny, max(nx - 1, 1))),
        dma((n,)), dma((nx, max(ny - 1, 1))),
        dma((max(ny - 1, 1),)), dma((max(ny - 1, 1),)),
        dma((max(nx - 1, 1),)), dma((max(nx - 1, 1),)),
        dma((2,)), dma((2,)), dma((2,)), dma((2,)),
        dma((2,)), dma((2,)), dma((2,)), dma((2,)),
        dma((4, max(nx, ny))), dma((4, max(nx, ny))),
        dma((1,)), dma((1,)),
    ]
    any_space = pl.BlockSpec(memory_space=pl.ANY)
    in_vmem = pl.BlockSpec(memory_space=pltpu.VMEM)
    merged, lhat, s, sown, inverse = pl.pallas_call(
        functools.partial(body, nx, ny, nz, 1.0 / n),
        out_shape=(
            jax.ShapeDtypeStruct((rows, total), F32),
            jax.ShapeDtypeStruct((rows, k), F32),
            jax.ShapeDtypeStruct((nx, ny, cb, k), F32),
            jax.ShapeDtypeStruct((cb, k), F32),
            jax.ShapeDtypeStruct((k, k), F32),
        ),
        in_specs=[in_vmem, any_space, any_space, any_space],
        out_specs=(any_space, in_vmem, any_space, in_vmem, in_vmem),
        scratch_shapes=scratch,
        compiler_params=pltpu.CompilerParams(
            collective_id=0, has_side_effects=True, vmem_limit_bytes=48 << 20
        ),
        name="compress",
    )(grad_out, activations, error_feedback, right_factor)
    s = s.reshape(n * cb, k)
    wide = min(512, total)
    return pl.pallas_call(
        finish_body,
        grid=(total // wide,),
        out_shape=(
            jax.ShapeDtypeStruct((1, rows, total), F32),
            jax.ShapeDtypeStruct((rows, total), jnp.bfloat16),
            jax.ShapeDtypeStruct((cb, k), F32),
        ),
        in_specs=[
            pl.BlockSpec((rows, wide), lambda i: (0, i)),
            pl.BlockSpec((rows, k), lambda i: (0, 0)),
            pl.BlockSpec((wide, k), lambda i: (i, 0)),
            pl.BlockSpec((rows, wide), lambda i: (0, i)),
            pl.BlockSpec((cb, k), lambda i: (0, 0)),
            pl.BlockSpec((k, k), lambda i: (0, 0)),
        ],
        out_specs=(
            pl.BlockSpec((1, rows, wide), lambda i: (0, 0, i)),
            pl.BlockSpec((rows, wide), lambda i: (0, i)),
            pl.BlockSpec((cb, k), lambda i: (0, 0)),
        ),
        name="finish",
    )(merged, lhat, s, momentum, sown, inverse)


def build(mesh, nx, ny, nz):
    return jax.shard_map(
        functools.partial(per_device, nx, ny, nz),
        mesh=mesh,
        in_specs=(
            P("dp", "rows"),
            P("dp", "rows"),
            P("dp", "rows", None),
            P("rows", None),
            P("rows", None),
        ),
        out_specs=(P("dp", "rows", None), P("rows", None), P("rows", None)),
        check_vma=False,
    )


def solution(mesh):
    return build(mesh, 4, 4, 8)
```

```python
import functools

import jax
import jax.numpy as jnp
from jax import lax
from jax.experimental import pallas as pl
from jax.experimental.pallas import tpu as pltpu
from jax.sharding import PartitionSpec as P

MOMENTUM_RATE = 0.9
HIGHEST = lax.Precision.HIGHEST
MESH = pl.DeviceIdType.MESH
F32 = jnp.float32
PANEL = 16
SCALE_ROWS = 16
LAG = 3
VMEM_LIMIT = 33_554_432


def dot32(a, b, dims=((1,), (0,))):
    return lax.dot_general(
        a, b, (dims, ((), ())), precision=HIGHEST, preferred_element_type=F32
    )


def ring_dist(delta, size):
    return min(delta, size - delta)


def far_first(n_a, n_b, weight):
    pairs = [(a, b) for a in range(n_a) for b in range(n_b) if a or b]
    return sorted(pairs, key=lambda p: -weight(*p))


def encode(v):
    peak = jnp.max(jnp.max(jnp.abs(v), axis=0, keepdims=True), axis=1, keepdims=True)
    peak = jnp.maximum(peak, 1e-30).astype(jnp.bfloat16).astype(F32)
    t = v * (1024.0 / peak)
    t4 = (t * t) * (t * t)
    t12 = t4 * t4 * t4
    code = jnp.where(v < 0, -t12, t12).astype(jnp.bfloat16)
    return code, jnp.broadcast_to(peak, (SCALE_ROWS, v.shape[1])).astype(jnp.bfloat16)


def decode(code, peak):
    y = code.astype(F32)
    size = jnp.abs(y)
    r = jnp.exp2(jnp.log2(jnp.maximum(size, 1e-37)) * (1.0 / 12.0) - 10.0)
    r = jnp.where(size > 1e-37, r, 0.0) * peak[:1].astype(F32)
    return jnp.where(y < 0, -r, r)


def cholesky_panels(aug, first, last):
    k = aug.shape[0]

    def panel(p, carry):
        base = pl.multiple_of(p * PANEL, PANEL)
        rows = aug[pl.ds(base, PANEL), :]
        lane = lax.broadcasted_iota(jnp.int32, (PANEL, 2 * k), 1)
        sub = lax.broadcasted_iota(jnp.int32, (PANEL, 1), 0)
        left = rows[:, :k]
        lane_k = lax.broadcasted_iota(jnp.int32, (PANEL, k), 1)
        cols = [
            jnp.sum(jnp.where(lane_k == base + i, left, 0.0), axis=1, keepdims=True)
            for i in range(PANEL)
        ]
        for i in range(PANEL):
            scale = lax.rsqrt(cols[i][i : i + 1, :])
            factor = jnp.where(sub > i, cols[i] * scale, 0.0)
            keep = sub == i
            head = rows[i : i + 1, :] * scale
            rows = jnp.where(keep, head, rows - factor * head)
            for m in range(i + 1, PANEL):
                cols[m] = cols[m] - factor * (cols[m][i : i + 1, :] * scale)
        aug[pl.ds(base, PANEL), :] = rows
        upper = jnp.where(lane_k >= base + PANEL, rows[:, :k], 0.0)
        aug[...] = aug[...] - dot32(upper.T, rows)
        return carry

    lax.fori_loop(first, last, panel, 0)


def body(
    nx, ny, nz, scale,
    grad, act, err, right0, momentum,
    merged, lhat_out, s_full, sown_out, inv_out, momentum_out,
    grad_v, act_all, grad_t, err_v, rb, m_tile, m_t,
    xt, yt, xr, yr, xs, ys, xf, yf, top, bottom,
    p_plane, r_plane, f_plane, p_col, r_col, f_col, aug,
    local_sem, up_send, up_recv, down_send, down_recv, sib_send, sib_recv,
    rb_send, rb_recv, x_send, x_recv, y_send, y_recv, xf_send, xf_recv, yf_send, yf_recv,
    ps_send, ps_recv, pg_send, pg_recv, cs_send, cs_recv, cg_send, cg_recv,
    ag_send, ag_recv, dd_send, dd_recv,
):
    d, j = lax.axis_index("dp"), lax.axis_index("rows")
    y, x = d // nx, d % nx
    z, c = j // 2, j % 2
    tok, cb = act.shape
    rb_rows = grad.shape[1]
    half_rows = rb_rows // 2
    n = nx * ny
    far = nz // 2
    th = tok // 2

    def plane_id(dy, dx):
        return (((y + dy) % ny) * nx + (x + dx) % nx, j)

    def col_id(dz, dc):
        return (d, ((z + dz) % nz) * 2 + (c + dc) % 2)

    plane = far_first(ny, nx, lambda a, b: ring_dist(a, ny) + ring_dist(b, nx))
    column = far_first(nz, 2, lambda a, b: ring_dist(a, nz) + 0.1 * b)

    def remote(src, dst, send, recv, device):
        return pltpu.make_async_remote_copy(
            src_ref=src, dst_ref=dst, send_sem=send, recv_sem=recv,
            device_id=device, device_id_type=MESH,
        )

    load_act = pltpu.make_async_copy(act, act_all.at[0, 0], local_sem.at[0])
    load_act.start()
    load_grad = pltpu.make_async_copy(grad, grad_v, local_sem.at[3])
    load_grad.start()
    load_err = pltpu.make_async_copy(err.at[0], err_v, local_sem.at[1])
    load_err.start()

    barrier = pltpu.get_barrier_semaphore()
    near = [plane_id(dy, 0) for dy in range(1, ny)] + [plane_id(0, dx) for dx in range(1, nx)]
    near += [col_id(dz, 0) for dz in sorted({1, nz - 1})] + [col_id(0, 1)]
    for device in near:
        pl.semaphore_signal(barrier, inc=1, device_id=device, device_id_type=MESH)
    load_act.wait()
    pl.semaphore_wait(barrier, len(near))

    pending = []

    def half(slot, h):
        return act_all.at[slot, 0, pl.ds(h * th, th)]

    def up(s, h):
        return remote(half((nz - s + 1) % nz, h), half(nz - s, h), up_send.at[s - 1, h], up_recv.at[s - 1, h], col_id(1, 0))

    def down(s, h):
        return remote(half(s - 1, h), half(s, h), down_send.at[s - 1, h], down_recv.at[s - 1, h], col_id(nz - 1, 0))

    def sibling(slot, h):
        return remote(half(slot, h), act_all.at[slot, 1, pl.ds(h * th, th)], sib_send.at[slot, h], sib_recv.at[slot, h], col_id(0, 1))

    up_list = [(s, h) for s in range(1, far) for h in (0, 1)] + [(far, 0)]
    down_list = [(s, h) for s in range(1, far) for h in (1, 0)] + [(far, 1)]

    def gather_sent():
        for s, h in up_list:
            up(s, h).wait_send()
        for s, h in down_list:
            down(s, h).wait_send()
        for slot in range(nz):
            for h in (0, 1):
                sibling(slot, h).wait_send()

    pending.append(gather_sent)
    for ua, da in zip(up_list[:2], down_list[:2]):
        if ua[0] == 1:
            up(*ua).start()
        if da[0] == 1:
            down(*da).start()
    for h in (0, 1):
        sibling(0, h).start()

    own_block = x * ny + y
    src_z, src_c = own_block // 2, own_block % 2
    rb_up = remote(rb, rb, rb_send.at[0], rb_recv, col_id(1, 0))
    rb_down = remote(rb, rb, rb_send.at[1], rb_recv, col_id(nz - 1, 0))
    rb_sib = remote(rb, rb, rb_send.at[2], rb_recv, col_id(0, 1))

    @pl.when(jnp.logical_and(z == src_z, c == src_c))
    def _():
        own = pltpu.make_async_copy(right0, rb, local_sem.at[2])
        own.start()
        own.wait()
        rb_up.start()
        if far > 1:
            rb_down.start()
        rb_sib.start()

    def rb_sent():
        away = (z - src_z + nz) % nz

        @pl.when(jnp.logical_and(c == src_c, away < far))
        def _():
            rb_up.wait_send()
        if far > 1:
            @pl.when(jnp.logical_and(c == src_c, jnp.logical_or(away == 0, away > far + 1)))
            def _():
                rb_down.wait_send()

        @pl.when(c == src_c)
        def _():
            rb_sib.wait_send()

    pending.append(rb_sent)

    def relay_rb(s, upward):
        at = (z - s) if upward else (z + s)

        @pl.when(jnp.logical_and((at + nz) % nz == src_z, c == src_c))
        def _():
            rb_up.wait_recv()
            if upward and s < far:
                rb_up.start()
            if not upward and s < far - 1:
                rb_down.start()
            rb_sib.start()

    load_grad.wait()
    grad_t[...] = grad_v[...].astype(F32).T.astype(jnp.bfloat16)
    load_err.wait()
    load_momentum = pltpu.make_async_copy(momentum, momentum_out, local_sem.at[1])
    load_momentum.start()
    pending.append(load_momentum.wait)
    def block_of(slot, dc):
        return ((z + slot) % nz) * 2 + (c + dc) % 2

    def columns(b):
        return pl.ds(pl.multiple_of(b * cb, cb), cb)

    def x_copy(b, dx, slot=0):
        return remote(xt.at[slot], xr.at[b % ny, dx - 1],
                      x_send.at[slot], x_recv.at[b % ny, dx - 1], plane_id(0, dx))

    def y_copy(b, dy, slot=0):
        return remote(yt.at[slot], yr.at[b // ny, dy - 1],
                      y_send.at[slot], y_recv.at[b // ny, dy - 1], plane_id(dy, 0))

    def put(ref, index, v):
        code, peak = encode(v)
        ref[index, :half_rows] = code
        ref[index, half_rows:] = peak

    def get(ref, *index):
        message = ref[index]
        return decode(message[:half_rows], message[half_rows:])

    def produce(slot, dc):
        if dc == 1:
            for h in (0, 1):
                sibling(slot, h).wait_recv()
        b = block_of(slot, dc)
        cols = columns(b)
        tile = jnp.dot(grad_t[...], act_all[slot, dc], preferred_element_type=F32) + err_v[:, cols]
        merged[:, cols] = tile
        owner_x, owner_y = b // ny, b % ny
        at = 2 * slot + dc
        if nx > 1:
            @pl.when(owner_x != x)
            def _():
                put(xt, at, tile[:half_rows])
                x_copy(b, (owner_x - x + nx) % nx, at).start()
        if ny > 1:
            @pl.when(owner_y != y)
            def _():
                put(yt, at, tile[half_rows:])
                y_copy(b, (owner_y - y + ny) % ny, at).start()

    def xf_copy(dy):
        return remote(xs.at[dy - 1], xf.at[dy - 1], xf_send.at[dy - 1], xf_recv.at[dy - 1], plane_id(dy, 0))

    def yf_copy(dx):
        return remote(ys.at[dx - 1], yf.at[dx - 1], yf_send.at[dx - 1], yf_recv.at[dx - 1], plane_id(0, dx))

    def consume(slot, dc):
        b = block_of(slot, dc)
        cols = columns(b)
        owner_x, owner_y = b // ny, b % ny

        @pl.when(owner_x == x)
        def _():
            total = merged[pl.ds(0, half_rows), cols]
            for dx in range(1, nx):
                x_copy(b, dx).wait_recv()
                total = total + get(xr, b % ny, dx - 1)

            @pl.when(owner_y == y)
            def _():
                top[...] = total

            @pl.when(owner_y != y)
            def _():
                dy = (owner_y - y + ny) % ny
                put(xs, dy - 1, total)
                xf_copy(dy).start()

        @pl.when(owner_y == y)
        def _():
            total = merged[pl.ds(half_rows, half_rows), cols]
            for dy in range(1, ny):
                y_copy(b, dy).wait_recv()
                total = total + get(yr, b // ny, dy - 1)

            @pl.when(owner_x == x)
            def _():
                bottom[...] = total

            @pl.when(owner_x != x)
            def _():
                dx = (owner_x - x + nx) % nx
                put(ys, dx - 1, total)
                yf_copy(dx).start()

    def tiles_sent():
        for slot in range(nz):
            for dc in (0, 1):
                b, at = block_of(slot, dc), 2 * slot + dc

                @pl.when(b // ny != x)
                def _(b=b, at=at):
                    x_copy(b, 1, at).wait_send()

                @pl.when(b % ny != y)
                def _(b=b, at=at):
                    y_copy(b, 1, at).wait_send()
        for dy in range(1, ny):
            xf_copy(dy).wait_send()
        for dx in range(1, nx):
            yf_copy(dx).wait_send()

    pending.append(tiles_sent)
    produce(0, 0)
    later = {i: [] for i in range(nz + 3)}
    later[0].append((0, 1))
    for i, ((s, h), (t, g)) in enumerate(zip(up_list, down_list)):
        if s < far and h == 1:
            later[i] += [(nz - s, 0), (s, 0), (nz - s, 1), (s, 1)]
        if s == far:
            later[i] += [(far, 0), (far, 1)]
    waiting = [[(0, 0)]]
    steps = len(up_list)
    for i in range(steps):
        (s, h), (t, g) = up_list[i], down_list[i]
        up(s, h).wait_recv()
        if s + 1 < far or (s + 1 == far and h == 0):
            up(s + 1, h).start()
        sibling(nz - s, h).start()
        down(t, g).wait_recv()
        if t + 1 < far or (t + 1 == far and g == 1):
            down(t + 1, g).start()
        sibling(t, g).start()
        if s == far or h == 1:
            relay_rb(s, True)
            if s < far:
                relay_rb(s, False)
        for slot, dc in later[i]:
            produce(slot, dc)
        waiting.append(later[i])
        if len(waiting) > LAG:
            for slot, dc in waiting.pop(0):
                consume(slot, dc)
    for group in waiting:
        for slot, dc in group:
            consume(slot, dc)

    @pl.when(c != src_c)
    def _():
        rb_sib.wait_recv()

    acc = top[...]
    for dy in range(1, ny):
        xf_copy(dy).wait_recv()
        acc = acc + get(xf, dy - 1)
    m_tile[pl.ds(0, half_rows), :] = acc * scale
    acc = bottom[...]
    for dx in range(1, nx):
        yf_copy(dx).wait_recv()
        acc = acc + get(yf, dx - 1)
    m_tile[pl.ds(half_rows, half_rows), :] = acc * scale

    sr = rb_rows // n
    gr = aug.shape[0] // n
    k = aug.shape[0]

    def wait_bytes(ref, sem):
        pltpu.make_async_copy(ref, ref, sem).wait()

    def plane_scatter(stage):
        pending.append(lambda: wait_bytes(r_plane.at[stage], ps_send.at[stage]))
        pending.append(lambda: wait_bytes(r_plane.at[stage], pg_send.at[stage]))
        for i, (dy, dx) in enumerate(plane):
            dev = plane_id(dy, dx)
            remote(p_plane.at[stage, dev[0]], r_plane.at[stage, i], ps_send.at[stage], ps_recv.at[stage], dev).start()

    def plane_gather(stage):
        wait_bytes(r_plane.at[stage], ps_recv.at[stage])
        total = p_plane[stage, d]
        for i in range(len(plane)):
            total = total + r_plane[stage, i]
        f_plane[stage, d] = total
        for dy, dx in plane:
            remote(f_plane.at[stage, d], f_plane.at[stage, d], pg_send.at[stage], pg_recv.at[stage], plane_id(dy, dx)).start()

    def plane_finish(stage):
        wait_bytes(r_plane.at[stage], pg_recv.at[stage])
        return f_plane[stage].reshape(rb_rows, k)

    def col_scatter(stage):
        pending.append(lambda: wait_bytes(r_col.at[stage], cs_send.at[stage]))
        pending.append(lambda: wait_bytes(r_col.at[stage], cg_send.at[stage]))
        for i, (dz, dc) in enumerate(column):
            dev = col_id(dz, dc)
            remote(p_col.at[stage, dev[1]], r_col.at[stage, i], cs_send.at[stage], cs_recv.at[stage], dev).start()

    def col_gather(stage):
        wait_bytes(r_col.at[stage], cs_recv.at[stage])
        total = p_col[stage, j]
        for i in range(len(column)):
            total = total + r_col[stage, i]
        f_col[stage, j] = total
        for dz, dc in column:
            remote(f_col.at[stage, j], f_col.at[stage, j], cg_send.at[stage], cg_recv.at[stage], col_id(dz, dc)).start()

    def col_finish(stage):
        wait_bytes(r_col.at[stage], cg_recv.at[stage])
        both = f_col[stage]
        return both[:, :sr].reshape(cb, k), both[:, sr:].reshape(k, k)

    def set_aug(gram):
        row = lax.broadcasted_iota(jnp.int32, (k, k), 0)
        col = lax.broadcasted_iota(jnp.int32, (k, k), 1)
        aug[:, :k] = gram
        aug[:, k:] = jnp.where(row == col, 1.0, 0.0).astype(F32)

    panels = k // PANEL

    p_plane[0] = dot32(m_tile[...], rb[...]).reshape(n, sr, k)
    plane_scatter(0)
    m_t[...] = m_tile[...].T
    plane_gather(0)
    left = plane_finish(0)
    p_col[0, :, :sr] = dot32(m_t[...], left).reshape(n, sr, k)
    p_col[0, :, sr:] = dot32(left, left, ((0,), (0,))).reshape(n, gr, k)
    col_scatter(0)
    col_gather(0)
    s_one, gram_one = col_finish(0)
    p_plane[1] = dot32(m_tile[...], s_one).reshape(n, sr, k)
    plane_scatter(1)
    set_aug(gram_one)
    cholesky_panels(aug, 0, panels // 2)
    plane_gather(1)
    cholesky_panels(aug, panels // 2, panels)
    left = dot32(plane_finish(1), aug[:, k:], ((1,), (1,)))
    p_col[1, :, :sr] = dot32(m_t[...], left).reshape(n, sr, k)
    p_col[1, :, sr:] = dot32(left, left, ((0,), (0,))).reshape(n, gr, k)
    col_scatter(1)
    col_gather(1)
    _, gram_two = col_finish(1)

    hc = cb // 2
    own_half = f_col[1, pl.ds(c * (n // 2), n // 2), :sr, :].reshape(hc, k)
    s_full[x, y, pl.ds(pl.multiple_of(c * hc, hc), hc), :] = own_half
    q = hc // 2
    q0 = pl.ds(pl.multiple_of(c * hc, hc), q)
    q1 = pl.ds(pl.multiple_of(c * hc + q, q), q)

    def ag1x(dx):
        ref = s_full.at[x, y, q0]
        return remote(ref, ref, ag_send.at[0, dx - 1], ag_recv.at[0, dx - 1], plane_id(0, dx))

    def ag1y(dy):
        ref = s_full.at[x, y, q1]
        return remote(ref, ref, ag_send.at[1, dy - 1], ag_recv.at[1, dy - 1], plane_id(dy, 0))

    def ag2x(dy):
        ref = s_full.at[:, y, q0]
        return remote(ref, ref, ag_send.at[2, dy - 1], ag_recv.at[2, dy - 1], plane_id(dy, 0))

    def ag2y(dx):
        ref = s_full.at[x, :, q1]
        return remote(ref, ref, ag_send.at[3, dx - 1], ag_recv.at[3, dx - 1], plane_id(0, dx))

    def d2d(i, where):
        ref = s_full.at[where]
        return remote(ref, ref, dd_send.at[i], dd_recv.at[i], col_id(0, 1))

    def right_sent():
        for dy in range(1, ny):
            ag1y(dy).wait_send()
            ag2x(dy).wait_send()
        for dx in range(1, nx):
            ag1x(dx).wait_send()
            ag2y(dx).wait_send()

    pending.append(right_sent)
    for dx in range(1, nx):
        ag1x(dx).start()
    for dy in range(1, ny):
        ag1y(dy).start()
    set_aug(gram_two)
    cholesky_panels(aug, 0, panels // 2)
    for dx in range(1, nx):
        ag1x(dx).wait_recv()
    for dy in range(1, ny):
        ag2x(dy).start()
    for dy in range(1, ny):
        ag1y(dy).wait_recv()
    for dx in range(1, nx):
        ag2y(dx).start()
    cholesky_panels(aug, panels // 2, panels)
    inverse = aug[:, k:]
    inv_out[...] = inverse
    lhat_out[...] = dot32(dot32(left, inverse, ((1,), (1,))), inverse)

    for dy in range(1, ny):
        ag2x(dy).wait_recv()
    for dx in range(1, nx):
        ag2y(dx).wait_recv()
    share = d2d(0, (slice(None), slice(None), pl.ds(pl.multiple_of(c * hc, hc), hc)))
    share.start()
    share.wait_recv()
    sown_out[...] = s_full[j // ny, j % ny]

    for wait in pending:
        wait()
    share.wait_send()


def split(v):
    high = v.astype(jnp.bfloat16)
    return high, (v - high.astype(F32)).astype(jnp.bfloat16)


def finish_body(wide, merged, lhat, s, momentum, sown, inverse, error, new_momentum, right, e_buf, m_buf, sem):
    total = merged.shape[1]
    l_high, l_low = split(lhat[...])
    l_all = jnp.concatenate([l_high, l_high, l_low], axis=1)

    def copies(i):
        cols = pl.ds(i * wide, wide)
        return (
            pltpu.make_async_copy(e_buf.at[i], error.at[0, :, cols], sem.at[i, 0]),
            pltpu.make_async_copy(m_buf.at[i], new_momentum.at[:, cols], sem.at[i, 1]),
        )

    for i in range(total // wide):
        cols = pl.ds(i * wide, wide)
        s_high, s_low = split(s[cols, :])
        s_all = jnp.concatenate([s_high, s_low, s_high], axis=1)
        approx = lax.dot_general(l_all, s_all, (((1,), (1,)), ((), ())), preferred_element_type=F32)
        e_buf[i] = merged[:, cols] - approx
        m_buf[i] = (MOMENTUM_RATE * momentum[:, cols].astype(F32) + approx).astype(jnp.bfloat16)
        for copy in copies(i):
            copy.start()
    right[...] = dot32(sown[...], inverse[...], ((1,), (1,)))
    for i in range(total // wide):
        for copy in copies(i):
            copy.wait()


def per_device(nx, ny, nz, grad_out, activations, error_feedback, momentum, right_factor):
    n = nx * ny
    tok, cb = activations.shape
    rows = grad_out.shape[1]
    total = error_feedback.shape[2]
    k = right_factor.shape[1]
    sr, gr, hr = rows // n, k // n, rows // 2
    far = nz // 2
    vmem, dma = pltpu.VMEM, pltpu.SemaphoreType.DMA
    scratch = [
        vmem((tok, rows), jnp.bfloat16),
        vmem((nz, 2, tok, cb), jnp.bfloat16),
        vmem((rows, tok), jnp.bfloat16),
        vmem((rows, total), F32),
        vmem((cb, k), F32),
        vmem((rows, cb), F32),
        vmem((cb, rows), F32),
        vmem((n, hr + SCALE_ROWS, cb), jnp.bfloat16),
        vmem((n, hr + SCALE_ROWS, cb), jnp.bfloat16),
        vmem((ny, max(nx - 1, 1), hr + SCALE_ROWS, cb), jnp.bfloat16),
        vmem((nx, max(ny - 1, 1), hr + SCALE_ROWS, cb), jnp.bfloat16),
        vmem((max(ny - 1, 1), hr + SCALE_ROWS, cb), jnp.bfloat16),
        vmem((max(nx - 1, 1), hr + SCALE_ROWS, cb), jnp.bfloat16),
        vmem((max(ny - 1, 1), hr + SCALE_ROWS, cb), jnp.bfloat16),
        vmem((max(nx - 1, 1), hr + SCALE_ROWS, cb), jnp.bfloat16),
        vmem((hr, cb), F32),
        vmem((hr, cb), F32),
        vmem((2, n, sr, k), F32),
        vmem((2, n - 1, sr, k), F32),
        vmem((2, n, sr, k), F32),
        vmem((2, n, sr + gr, k), F32),
        vmem((2, n - 1, sr + gr, k), F32),
        vmem((2, n, sr + gr, k), F32),
        vmem((k, 2 * k), F32),
        dma((4,)),
        dma((far, 2)), dma((far, 2)), dma((far, 2)), dma((far, 2)),
        dma((nz, 2)), dma((nz, 2)),
        dma((3,)), dma,
        dma((n,)), dma((ny, max(nx - 1, 1))),
        dma((n,)), dma((nx, max(ny - 1, 1))),
        dma((max(ny - 1, 1),)), dma((max(ny - 1, 1),)),
        dma((max(nx - 1, 1),)), dma((max(nx - 1, 1),)),
        dma((2,)), dma((2,)), dma((2,)), dma((2,)),
        dma((2,)), dma((2,)), dma((2,)), dma((2,)),
        dma((4, max(nx, ny))), dma((4, max(nx, ny))),
        dma((1,)), dma((1,)),
    ]
    any_space = pl.BlockSpec(memory_space=pl.ANY)
    in_vmem = pl.BlockSpec(memory_space=pltpu.VMEM)
    merged, lhat, s, sown, inverse, momentum = pl.pallas_call(
        functools.partial(body, nx, ny, nz, 1.0 / n),
        out_shape=(
            jax.ShapeDtypeStruct((rows, total), F32),
            jax.ShapeDtypeStruct((rows, k), F32),
            jax.ShapeDtypeStruct((nx, ny, cb, k), F32),
            jax.ShapeDtypeStruct((cb, k), F32),
            jax.ShapeDtypeStruct((k, k), F32),
            jax.ShapeDtypeStruct((rows, total), momentum.dtype),
        ),
        in_specs=[any_space] * 5,
        out_specs=(in_vmem,) * 6,
        scratch_shapes=scratch,
        compiler_params=pltpu.CompilerParams(
            collective_id=0, has_side_effects=True, vmem_limit_bytes=VMEM_LIMIT
        ),
        name="compress",
    )(*[pltpu.with_memory_space_constraint(v, pltpu.HBM) for v in (grad_out, activations, error_feedback, right_factor, momentum)])
    s = s.reshape(n * cb, k)
    wide = min(512, total)
    return pl.pallas_call(
        functools.partial(finish_body, wide),
        out_shape=(
            jax.ShapeDtypeStruct((1, rows, total), F32),
            jax.ShapeDtypeStruct((rows, total), jnp.bfloat16),
            jax.ShapeDtypeStruct((cb, k), F32),
        ),
        in_specs=[in_vmem] * 6,
        out_specs=(any_space, any_space, in_vmem),
        scratch_shapes=[
            vmem((total // wide, rows, wide), F32),
            vmem((total // wide, rows, wide), jnp.bfloat16),
            dma((total // wide, 2)),
        ],
        compiler_params=pltpu.CompilerParams(vmem_limit_bytes=20 << 20),
        name="finish",
    )(merged, lhat, s, momentum, sown, inverse)


def build(mesh, nx, ny, nz):
    return jax.shard_map(
        functools.partial(per_device, nx, ny, nz),
        mesh=mesh,
        in_specs=(
            P("dp", "rows"),
            P("dp", "rows"),
            P("dp", "rows", None),
            P("rows", None),
            P("rows", None),
        ),
        out_specs=(P("dp", "rows", None), P("rows", None), P("rows", None)),
        check_vma=False,
    )


def solution(mesh):
    return build(mesh, 4, 4, 8)
```

```python
import functools

import jax
import jax.numpy as jnp
from jax import lax
from jax.experimental import pallas as pl
from jax.experimental.pallas import tpu as pltpu
from jax.sharding import PartitionSpec as P

MOMENTUM_RATE = 0.9
HIGHEST = lax.Precision.HIGHEST
MESH = pl.DeviceIdType.MESH
F32 = jnp.float32
PANEL = 16
SCALE_ROWS = 16
LAG = 5
PARTS = 4
VMEM_LIMIT = 33_554_432


def dot32(a, b, dims=((1,), (0,))):
    return lax.dot_general(
        a, b, (dims, ((), ())), precision=HIGHEST, preferred_element_type=F32
    )


def ring_dist(delta, size):
    return min(delta, size - delta)


def far_first(n_a, n_b, weight):
    pairs = [(a, b) for a in range(n_a) for b in range(n_b) if a or b]
    return sorted(pairs, key=lambda p: -weight(*p))


def encode(v):
    peak = jnp.max(jnp.max(jnp.abs(v), axis=0, keepdims=True), axis=1, keepdims=True)
    peak = jnp.maximum(peak, 1e-30).astype(jnp.bfloat16).astype(F32)
    t = v * (128.0 / peak)
    t4 = (t * t) * (t * t)
    t8 = t4 * t4
    t16 = t8 * t8
    code = jnp.where(v < 0, -t16, t16).astype(jnp.bfloat16)
    return code, jnp.broadcast_to(peak, (SCALE_ROWS, v.shape[1])).astype(jnp.bfloat16)


def decode(code, peak):
    y = code.astype(F32)
    size = jnp.abs(y)
    r = jnp.exp2(jnp.log2(jnp.maximum(size, 1e-37)) * (1.0 / 16.0) - 7.0)
    r = jnp.where(size > 1e-37, r, 0.0) * peak[:1].astype(F32)
    return jnp.where(y < 0, -r, r)


def split(v):
    high = v.astype(jnp.bfloat16)
    return high, (v - high.astype(F32)).astype(jnp.bfloat16)


def dot_split(a, b):
    a_high, a_low = split(a)
    b_high, b_low = split(b)
    return jnp.dot(
        jnp.concatenate([a_high, a_high, a_low], axis=1),
        jnp.concatenate([b_high, b_low, b_high], axis=0),
        preferred_element_type=F32,
    )


def cholesky_panels(aug, first, last):
    k = aug.shape[0]

    def panel(p, carry):
        base = pl.multiple_of(p * PANEL, PANEL)
        rows = aug[pl.ds(base, PANEL), :]
        lane = lax.broadcasted_iota(jnp.int32, (PANEL, 2 * k), 1)
        sub = lax.broadcasted_iota(jnp.int32, (PANEL, 1), 0)
        left = rows[:, :k]
        lane_k = lax.broadcasted_iota(jnp.int32, (PANEL, k), 1)
        cols = [
            jnp.sum(jnp.where(lane_k == base + i, left, 0.0), axis=1, keepdims=True)
            for i in range(PANEL)
        ]
        for i in range(PANEL):
            scale = lax.rsqrt(cols[i][i : i + 1, :])
            factor = jnp.where(sub > i, cols[i] * scale, 0.0)
            keep = sub == i
            head = rows[i : i + 1, :] * scale
            rows = jnp.where(keep, head, rows - factor * head)
            for m in range(i + 1, PANEL):
                cols[m] = cols[m] - factor * (cols[m][i : i + 1, :] * scale)
        aug[pl.ds(base, PANEL), :] = rows
        upper = jnp.where(lane_k >= base + PANEL, rows[:, :k], 0.0)
        aug[...] = aug[...] - dot32(upper.T, rows)
        return carry

    lax.fori_loop(first, last, panel, 0)


def body(
    nx, ny, nz, scale,
    grad, act, err, right0, momentum,
    merged, lhat_out, s_full, sown_out, inv_out, momentum_out,
    grad_v, act_all, grad_t, err_v, r_all, m_tile, m_t,
    xt, yt, xr, yr, xs, ys, xf, yf, top, bottom,
    p_plane, r_plane, f_plane, p_col, r_col, f_col, p_gram, r_gram, f_gram, aug,
    local_sem, up_send, up_recv, down_send, down_recv, sib_send, sib_recv,
    rs_send, rs_recv, x_send, x_recv, y_send, y_recv, xf_send, xf_recv, yf_send, yf_recv,
    ps_send, ps_recv, pg_send, pg_recv, cs_send, cs_recv, cg_send, cg_recv, gs_send, gs_recv, gg_send, gg_recv,
    ag_send, ag_recv, dd_send, dd_recv,
):
    d, j = lax.axis_index("dp"), lax.axis_index("rows")
    y, x = d // nx, d % nx
    z, c = j // 2, j % 2
    tok, cb = act.shape
    rb_rows = grad.shape[1]
    half_rows = rb_rows // 2
    n = nx * ny
    far = nz // 2
    th = tok // PARTS

    def plane_id(dy, dx):
        return (((y + dy) % ny) * nx + (x + dx) % nx, j)

    def col_id(dz, dc):
        return (d, ((z + dz) % nz) * 2 + (c + dc) % 2)

    plane = far_first(ny, nx, lambda a, b: ring_dist(a, ny) + ring_dist(b, nx))
    column = far_first(nz, 2, lambda a, b: ring_dist(a, nz) + 0.1 * b)

    def remote(src, dst, send, recv, device):
        return pltpu.make_async_remote_copy(
            src_ref=src, dst_ref=dst, send_sem=send, recv_sem=recv,
            device_id=device, device_id_type=MESH,
        )

    load_act = pltpu.make_async_copy(act, act_all.at[0, 0], local_sem.at[0])
    load_act.start()
    load_grad = pltpu.make_async_copy(grad, grad_v, local_sem.at[3])
    load_grad.start()
    load_err = pltpu.make_async_copy(err.at[0], err_v, local_sem.at[1])
    load_err.start()

    barrier = pltpu.get_barrier_semaphore()
    near = [plane_id(dy, 0) for dy in range(1, ny)] + [plane_id(0, dx) for dx in range(1, nx)]
    near += [col_id(dz, 0) for dz in range(1, nz)] + [col_id(0, 1)]
    for device in near:
        pl.semaphore_signal(barrier, inc=1, device_id=device, device_id_type=MESH)
    sr = rb_rows // n
    gr = aug.shape[0] // n
    k = aug.shape[0]
    load_right = pltpu.make_async_copy(right0.at[pl.ds(pl.multiple_of(d * sr, sr), sr)], r_all.at[x, y, c, z], local_sem.at[2])
    load_right.start()
    load_act.wait()
    load_right.wait()
    pl.semaphore_wait(barrier, len(near))

    pending = []

    def wait_bytes(ref, sem):
        pltpu.make_async_copy(ref, ref, sem).wait()

    far_z = sorted(range(1, nz), key=lambda dz: -ring_dist(dz, nz))

    class Everywhere:
        def __init__(self, buf, which):
            self.buf, self.which = buf, which
            half = nz // 2
            self.q = (pl.ds(0, half), pl.ds(half, nz - half))
            pending.append(self.sent)

        def column_start(self):
            ref = self.buf.at[x, y, c, z]
            for dz in far_z:
                remote(ref, ref, rs_send.at[self.which], rs_recv.at[self.which], col_id(dz, 0)).start()

        def column_wait(self):
            wait_bytes(self.buf.at[x, y, c, pl.ds(0, nz - 1)], rs_recv.at[self.which])

        def move(self, step, delta):
            q = self.q[step % 2]
            at = (x, y) if step < 2 else ((slice(None), y) if step == 2 else (x, slice(None)))
            ref = self.buf.at[at[0], at[1], c, q]
            along_x = step in (0, 3)
            return remote(ref, ref, ag_send.at[self.which, step, delta - 1], ag_recv.at[self.which, step, delta - 1],
                          plane_id(0, delta) if along_x else plane_id(delta, 0))

        def share(self, i):
            if i < ny:
                ref = self.buf.at[:, (y - i + ny) % ny, c, self.q[0]]
            else:
                ref = self.buf.at[(x - (i - ny) + nx) % nx, :, c, self.q[1]]
            return remote(ref, ref, dd_send.at[self.which, i], dd_recv.at[self.which, i], col_id(0, 1))

        def first(self):
            for dx in range(1, nx):
                self.move(0, dx).start()
            for dy in range(1, ny):
                self.move(1, dy).start()

        def second(self):
            for dx in range(1, nx):
                self.move(0, dx).wait_recv()
            for dy in range(1, ny):
                self.move(2, dy).start()
            for dy in range(1, ny):
                self.move(1, dy).wait_recv()
            for dx in range(1, nx):
                self.move(3, dx).start()
            self.share(0).start()
            self.share(ny).start()

        def third(self):
            for i in range(1, max(nx, ny)):
                if i < ny:
                    self.move(2, i).wait_recv()
                    self.share(i).start()
                if i < nx:
                    self.move(3, i).wait_recv()
                    self.share(ny + i).start()

        def last(self):
            for i in range(nx + ny):
                self.share(i).wait_recv()

        def sent(self):
            wait_bytes(self.buf.at[x, y, c, pl.ds(0, nz - 1)], rs_send.at[self.which])
            for step in range(4):
                for delta in range(1, nx if step in (0, 3) else ny):
                    self.move(step, delta).wait_send()
            for i in range(nx + ny):
                self.share(i).wait_send()

    right_in = Everywhere(r_all, 0)
    right_out = Everywhere(s_full, 1)
    right_in.column_start()

    def half(slot, h):
        return act_all.at[slot, 0, pl.ds(h * th, th)]

    def up(s, h):
        return remote(half((nz - s + 1) % nz, h), half(nz - s, h), up_send.at[s - 1, h], up_recv.at[s - 1, h], col_id(1, 0))

    def down(s, h):
        return remote(half(s - 1, h), half(s, h), down_send.at[s - 1, h], down_recv.at[s - 1, h], col_id(nz - 1, 0))

    def sibling(slot, h):
        return remote(half(slot, h), act_all.at[slot, 1, pl.ds(h * th, th)], sib_send.at[slot, h], sib_recv.at[slot, h], col_id(0, 1))

    mid = PARTS // 2
    up_list = [(s, h) for s in range(1, far) for h in range(PARTS)] + [(far, h) for h in range(mid)]
    down_list = [(s, PARTS - 1 - h) for s, h in up_list]

    def gather_sent():
        for s, h in up_list:
            up(s, h).wait_send()
        for s, h in down_list:
            down(s, h).wait_send()
        for slot in range(nz):
            for h in range(PARTS):
                sibling(slot, h).wait_send()

    pending.append(gather_sent)
    for ua, da in zip(up_list[:PARTS], down_list[:PARTS]):
        up(*ua).start()
        down(*da).start()
    for h in range(PARTS):
        sibling(0, h).start()

    load_grad.wait()
    grad_t[...] = grad_v[...].astype(F32).T.astype(jnp.bfloat16)
    load_err.wait()
    load_momentum = pltpu.make_async_copy(momentum, momentum_out, local_sem.at[1])
    load_momentum.start()
    pending.append(load_momentum.wait)
    def block_of(slot, dc):
        return ((z + slot) % nz) * 2 + (c + dc) % 2

    def columns(b):
        return pl.ds(pl.multiple_of(b * cb, cb), cb)

    def x_copy(b, dx, slot=0):
        return remote(xt.at[slot], xr.at[b % ny, dx - 1],
                      x_send.at[slot], x_recv.at[b % ny, dx - 1], plane_id(0, dx))

    def y_copy(b, dy, slot=0):
        return remote(yt.at[slot], yr.at[b // ny, dy - 1],
                      y_send.at[slot], y_recv.at[b // ny, dy - 1], plane_id(dy, 0))

    def put(ref, index, v):
        code, peak = encode(v)
        ref[index, :half_rows] = code
        ref[index, half_rows:] = peak

    def get(ref, *index):
        message = ref[index]
        return decode(message[:half_rows], message[half_rows:])

    def produce(slot, dc):
        if dc == 1:
            for h in range(PARTS):
                sibling(slot, h).wait_recv()
        b = block_of(slot, dc)
        cols = columns(b)
        tile = jnp.dot(grad_t[...], act_all[slot, dc], preferred_element_type=F32) + err_v[:, cols]
        merged[:, cols] = tile
        owner_x, owner_y = b // ny, b % ny
        at = 2 * slot + dc
        if nx > 1:
            @pl.when(owner_x != x)
            def _():
                put(xt, at, tile[:half_rows])
                x_copy(b, (owner_x - x + nx) % nx, at).start()
        if ny > 1:
            @pl.when(owner_y != y)
            def _():
                put(yt, at, tile[half_rows:])
                y_copy(b, (owner_y - y + ny) % ny, at).start()

    def xf_copy(dy):
        return remote(xs.at[dy - 1], xf.at[dy - 1], xf_send.at[dy - 1], xf_recv.at[dy - 1], plane_id(dy, 0))

    def yf_copy(dx):
        return remote(ys.at[dx - 1], yf.at[dx - 1], yf_send.at[dx - 1], yf_recv.at[dx - 1], plane_id(0, dx))

    def consume(slot, dc):
        b = block_of(slot, dc)
        cols = columns(b)
        owner_x, owner_y = b // ny, b % ny

        @pl.when(owner_x == x)
        def _():
            total = merged[pl.ds(0, half_rows), cols]
            for dx in range(1, nx):
                x_copy(b, dx).wait_recv()
                total = total + get(xr, b % ny, dx - 1)

            @pl.when(owner_y == y)
            def _():
                top[...] = total

            @pl.when(owner_y != y)
            def _():
                dy = (owner_y - y + ny) % ny
                put(xs, dy - 1, total)
                xf_copy(dy).start()

        @pl.when(owner_y == y)
        def _():
            total = merged[pl.ds(half_rows, half_rows), cols]
            for dy in range(1, ny):
                y_copy(b, dy).wait_recv()
                total = total + get(yr, b // ny, dy - 1)

            @pl.when(owner_x == x)
            def _():
                bottom[...] = total

            @pl.when(owner_x != x)
            def _():
                dx = (owner_x - x + nx) % nx
                put(ys, dx - 1, total)
                yf_copy(dx).start()

    def tiles_sent():
        for slot in range(nz):
            for dc in (0, 1):
                b, at = block_of(slot, dc), 2 * slot + dc

                @pl.when(b // ny != x)
                def _(b=b, at=at):
                    x_copy(b, 1, at).wait_send()

                @pl.when(b % ny != y)
                def _(b=b, at=at):
                    y_copy(b, 1, at).wait_send()
        for dy in range(1, ny):
            xf_copy(dy).wait_send()
        for dx in range(1, nx):
            yf_copy(dx).wait_send()

    def multiply(pairs):
        total = jnp.zeros((rb_rows, k), F32)
        for slot, dc in pairs:
            b = block_of(slot, dc)
            strips = [r_all[i, h, b % 2, b // 2] for h in range(ny) for i in range(nx)]
            total = total + dot_split(merged[:, columns(b)], jnp.concatenate(strips, axis=0))
        return total

    def plane_scatter(stage):
        pending.append(lambda: wait_bytes(r_plane.at[stage], ps_send.at[stage]))
        pending.append(lambda: wait_bytes(r_plane.at[stage], pg_send.at[stage]))
        for i, (dy, dx) in enumerate(plane):
            dev = plane_id(dy, dx)
            remote(p_plane.at[stage, dev[0]], r_plane.at[stage, i], ps_send.at[stage], ps_recv.at[stage], dev).start()

    def plane_gather(stage):
        wait_bytes(r_plane.at[stage], ps_recv.at[stage])
        total = p_plane[stage, d]
        for i in range(len(plane)):
            total = total + r_plane[stage, i]
        f_plane[stage, d] = total
        for dy, dx in plane:
            remote(f_plane.at[stage, d], f_plane.at[stage, d], pg_send.at[stage], pg_recv.at[stage], plane_id(dy, dx)).start()

    def plane_finish(stage):
        wait_bytes(r_plane.at[stage], pg_recv.at[stage])
        return f_plane[stage].reshape(rb_rows, k)

    pending.append(tiles_sent)
    produce(0, 0)
    later = [[] for _ in range(len(up_list) + 1)]
    later[0].append((0, 1))
    for i, (s, h) in enumerate(up_list):
        if s < far and h == PARTS - 1:
            later[i] += [(nz - s, 0), (s, 0)]
            later[i + 1] += [(nz - s, 1), (s, 1)]
    later[len(up_list) - 1] += [(far, 0), (far, 1)]
    waiting = [[(0, 0)]]
    steps = len(up_list)
    multiplied = []
    for i, ((s, h), (t, g)) in enumerate(zip(up_list, down_list)):
        up(s, h).wait_recv()
        if s + 1 < far or (s + 1 == far and h < mid):
            up(s + 1, h).start()
        sibling(nz - s, h).start()
        down(t, g).wait_recv()
        if t + 1 < far or (t + 1 == far and g >= mid):
            down(t + 1, g).start()
        sibling(t, g).start()
        if i == min(2, steps - 1):
            right_in.column_wait()
            right_in.first()
        if i == min(6, steps - 1):
            right_in.second()
        if i == min(11, steps - 1):
            right_in.third()
        for slot, dc in later[i]:
            produce(slot, dc)
        waiting.append(later[i])
        if len(waiting) > LAG:
            for slot, dc in waiting.pop(0):
                consume(slot, dc)
        if i == max(steps - 2, min(11, steps - 1)):
            right_in.last()
            multiplied = [(0, 0)] + [pair for group in later[: i + 1] for pair in group]
            left_sum = multiply(multiplied)
    rest = [pair for group in later for pair in group if pair not in multiplied]
    p_plane[0] = ((left_sum + multiply(rest)) * scale).reshape(n, sr, k)
    plane_scatter(0)
    for group in waiting:
        for slot, dc in group:
            consume(slot, dc)
    plane_gather(0)

    acc = top[...]
    for dy in range(1, ny):
        xf_copy(dy).wait_recv()
        acc = acc + get(xf, dy - 1)
    m_tile[pl.ds(0, half_rows), :] = acc * scale
    acc = bottom[...]
    for dx in range(1, nx):
        yf_copy(dx).wait_recv()
        acc = acc + get(yf, dx - 1)
    m_tile[pl.ds(half_rows, half_rows), :] = acc * scale

    factor_col = (p_col, r_col, f_col, cs_send, cs_recv, cg_send, cg_recv)
    gram_col = (p_gram, r_gram, f_gram, gs_send, gs_recv, gg_send, gg_recv)

    def col_scatter(stage, what, both=True):
        part, got, full, s_send, s_recv, g_send, g_recv = what
        pending.append(lambda: wait_bytes(got.at[stage], s_send.at[stage]))
        if both:
            pending.append(lambda: wait_bytes(got.at[stage], g_send.at[stage]))
        for i, (dz, dc) in enumerate(column):
            dev = col_id(dz, dc)
            remote(part.at[stage, dev[1]], got.at[stage, i], s_send.at[stage], s_recv.at[stage], dev).start()

    def col_total(stage, what):
        part, got, full, s_send, s_recv, g_send, g_recv = what
        wait_bytes(got.at[stage], s_recv.at[stage])
        total = part[stage, j]
        for i in range(len(column)):
            total = total + got[stage, i]
        return total

    def col_gather(stage, what):
        part, got, full, s_send, s_recv, g_send, g_recv = what
        full[stage, j] = col_total(stage, what)
        for dz, dc in column:
            remote(full.at[stage, j], full.at[stage, j], g_send.at[stage], g_recv.at[stage], col_id(dz, dc)).start()

    def col_finish(stage, what):
        part, got, full, s_send, s_recv, g_send, g_recv = what
        wait_bytes(got.at[stage], g_recv.at[stage])
        return full[stage].reshape(-1, k)

    def right_of(stage, left):
        p_col[stage] = dot32(m_t[...], left).reshape(n, sr, k)
        col_scatter(stage, factor_col, stage == 0)
        p_gram[stage] = dot32(left, left, ((0,), (0,))).reshape(n, gr, k)
        col_scatter(stage, gram_col)
        if stage == 0:
            col_gather(stage, factor_col)
        else:
            s_full[x, y, c, z] = col_total(stage, factor_col)
            right_out.column_start()
        col_gather(stage, gram_col)

    def set_aug(gram):
        row = lax.broadcasted_iota(jnp.int32, (k, k), 0)
        col = lax.broadcasted_iota(jnp.int32, (k, k), 1)
        aug[:, :k] = gram
        aug[:, k:] = jnp.where(row == col, 1.0, 0.0).astype(F32)

    panels = k // PANEL

    m_t[...] = m_tile[...].T
    left = plane_finish(0)
    right_of(0, left)
    s_one = col_finish(0, factor_col)
    p_plane[1] = dot32(m_tile[...], s_one).reshape(n, sr, k)
    plane_scatter(1)
    set_aug(col_finish(0, gram_col))
    cholesky_panels(aug, 0, panels // 2)
    plane_gather(1)
    cholesky_panels(aug, panels // 2, panels)
    left = dot32(plane_finish(1), aug[:, k:], ((1,), (1,)))
    right_of(1, left)

    right_out.column_wait()
    right_out.first()
    set_aug(col_finish(1, gram_col))
    cholesky_panels(aug, 0, panels // 2)
    right_out.second()
    cholesky_panels(aug, panels // 2, panels)
    inverse = aug[:, k:]
    inv_out[...] = inverse
    lhat_out[...] = dot32(dot32(left, inverse, ((1,), (1,))), inverse)
    right_out.third()
    right_out.last()
    sown_out[...] = ordered(s_full, j // ny, j % ny)

    for wait in pending:
        wait()


def ordered(ref, *index):
    cores, depth = ref.shape[-4], ref.shape[-3]
    return jnp.concatenate([ref[(*index, c, z)] for z in range(depth) for c in range(cores)], axis=0)


def rows_of(ref):
    return ref.shape[1] * ref.shape[2] * ref.shape[3]


def finish_body(wide, merged, lhat, s, momentum, sown, inverse, error, new_momentum, right, e_buf, m_buf, sem):
    total = merged.shape[1]
    l_high, l_low = split(lhat[...])
    l_all = jnp.concatenate([l_high, l_high, l_low], axis=1)

    def copies(i):
        cols = pl.ds(i * wide, wide)
        return (
            pltpu.make_async_copy(e_buf.at[i], error.at[0, :, cols], sem.at[i, 0]),
            pltpu.make_async_copy(m_buf.at[i], new_momentum.at[:, cols], sem.at[i, 1]),
        )

    for i in range(total // wide):
        cols = pl.ds(i * wide, wide)
        blocks = wide // rows_of(s)
        s_high, s_low = split(jnp.concatenate([ordered(s, i * blocks + h) for h in range(blocks)], axis=0))
        s_all = jnp.concatenate([s_high, s_low, s_high], axis=1)
        approx = lax.dot_general(l_all, s_all, (((1,), (1,)), ((), ())), preferred_element_type=F32)
        e_buf[i] = merged[:, cols] - approx
        m_buf[i] = (MOMENTUM_RATE * momentum[:, cols].astype(F32) + approx).astype(jnp.bfloat16)
        for copy in copies(i):
            copy.start()
    right[...] = dot32(sown[...], inverse[...], ((1,), (1,)))
    for i in range(total // wide):
        for copy in copies(i):
            copy.wait()


def per_device(nx, ny, nz, grad_out, activations, error_feedback, momentum, right_factor):
    n = nx * ny
    tok, cb = activations.shape
    rows = grad_out.shape[1]
    total = error_feedback.shape[2]
    k = right_factor.shape[1]
    sr, gr, hr = rows // n, k // n, rows // 2
    far = nz // 2
    vmem, dma = pltpu.VMEM, pltpu.SemaphoreType.DMA
    scratch = [
        vmem((tok, rows), jnp.bfloat16),
        vmem((nz, 2, tok, cb), jnp.bfloat16),
        vmem((rows, tok), jnp.bfloat16),
        vmem((rows, total), F32),
        vmem((nx, ny, 2, nz, sr, k), F32),
        vmem((rows, cb), F32),
        vmem((cb, rows), F32),
        vmem((n, hr + SCALE_ROWS, cb), jnp.bfloat16),
        vmem((n, hr + SCALE_ROWS, cb), jnp.bfloat16),
        vmem((ny, max(nx - 1, 1), hr + SCALE_ROWS, cb), jnp.bfloat16),
        vmem((nx, max(ny - 1, 1), hr + SCALE_ROWS, cb), jnp.bfloat16),
        vmem((max(ny - 1, 1), hr + SCALE_ROWS, cb), jnp.bfloat16),
        vmem((max(nx - 1, 1), hr + SCALE_ROWS, cb), jnp.bfloat16),
        vmem((max(ny - 1, 1), hr + SCALE_ROWS, cb), jnp.bfloat16),
        vmem((max(nx - 1, 1), hr + SCALE_ROWS, cb), jnp.bfloat16),
        vmem((hr, cb), F32),
        vmem((hr, cb), F32),
        vmem((2, n, sr, k), F32),
        vmem((2, n - 1, sr, k), F32),
        vmem((2, n, sr, k), F32),
        vmem((2, n, sr, k), F32),
        vmem((2, n - 1, sr, k), F32),
        vmem((2, n, sr, k), F32),
        vmem((2, n, gr, k), F32),
        vmem((2, n - 1, gr, k), F32),
        vmem((2, n, gr, k), F32),
        vmem((k, 2 * k), F32),
        dma((4,)),
        dma((far, PARTS)), dma((far, PARTS)), dma((far, PARTS)), dma((far, PARTS)),
        dma((nz, PARTS)), dma((nz, PARTS)),
        dma((2,)), dma((2,)),
        dma((n,)), dma((ny, max(nx - 1, 1))),
        dma((n,)), dma((nx, max(ny - 1, 1))),
        dma((max(ny - 1, 1),)), dma((max(ny - 1, 1),)),
        dma((max(nx - 1, 1),)), dma((max(nx - 1, 1),)),
        dma((2,)), dma((2,)), dma((2,)), dma((2,)),
        dma((2,)), dma((2,)), dma((2,)), dma((2,)),
        dma((2,)), dma((2,)), dma((2,)), dma((2,)),
        dma((2, 4, max(nx, ny))), dma((2, 4, max(nx, ny))),
        dma((2, nx + ny)), dma((2, nx + ny)),
    ]
    any_space = pl.BlockSpec(memory_space=pl.ANY)
    in_vmem = pl.BlockSpec(memory_space=pltpu.VMEM)
    merged, lhat, s, sown, inverse, momentum = pl.pallas_call(
        functools.partial(body, nx, ny, nz, 1.0 / n),
        out_shape=(
            jax.ShapeDtypeStruct((rows, total), F32),
            jax.ShapeDtypeStruct((rows, k), F32),
            jax.ShapeDtypeStruct((nx, ny, 2, nz, sr, k), F32),
            jax.ShapeDtypeStruct((cb, k), F32),
            jax.ShapeDtypeStruct((k, k), F32),
            jax.ShapeDtypeStruct((rows, total), momentum.dtype),
        ),
        in_specs=[any_space] * 5,
        out_specs=(in_vmem,) * 6,
        scratch_shapes=scratch,
        compiler_params=pltpu.CompilerParams(
            collective_id=0, has_side_effects=True, vmem_limit_bytes=VMEM_LIMIT
        ),
        name="compress",
    )(*[pltpu.with_memory_space_constraint(v, pltpu.HBM) for v in (grad_out, activations, error_feedback, right_factor, momentum)])
    s = s.reshape(n, 2, nz, sr, k)
    wide = min(512, total)
    return pl.pallas_call(
        functools.partial(finish_body, wide),
        out_shape=(
            jax.ShapeDtypeStruct((1, rows, total), F32),
            jax.ShapeDtypeStruct((rows, total), jnp.bfloat16),
            jax.ShapeDtypeStruct((cb, k), F32),
        ),
        in_specs=[in_vmem] * 6,
        out_specs=(any_space, any_space, in_vmem),
        scratch_shapes=[
            vmem((total // wide, rows, wide), F32),
            vmem((total // wide, rows, wide), jnp.bfloat16),
            dma((total // wide, 2)),
        ],
        compiler_params=pltpu.CompilerParams(vmem_limit_bytes=20 << 20),
        name="finish",
    )(merged, lhat, s, momentum, sown, inverse)


def build(mesh, nx, ny, nz):
    return jax.shard_map(
        functools.partial(per_device, nx, ny, nz),
        mesh=mesh,
        in_specs=(
            P("dp", "rows"),
            P("dp", "rows"),
            P("dp", "rows", None),
            P("rows", None),
            P("rows", None),
        ),
        out_specs=(P("dp", "rows", None), P("rows", None), P("rows", None)),
        check_vma=False,
    )


def solution(mesh):
    return build(mesh, 4, 4, 8)
```

```python
import functools

import jax
import jax.numpy as jnp
from jax import lax
from jax.experimental import pallas as pl
from jax.experimental.pallas import tpu as pltpu
from jax.sharding import PartitionSpec as P

MOMENTUM_RATE = 0.9
HIGHEST = lax.Precision.HIGHEST
MESH = pl.DeviceIdType.MESH
F32 = jnp.float32
PANEL = 16
SCALE_ROWS = 16
PARTS = 4
VMEM_LIMIT = 33_554_432


def dot32(a, b, dims=((1,), (0,))):
    return lax.dot_general(
        a, b, (dims, ((), ())), precision=HIGHEST, preferred_element_type=F32
    )


def ring_dist(delta, size):
    return min(delta, size - delta)


def far_first(n_a, n_b, weight):
    pairs = [(a, b) for a in range(n_a) for b in range(n_b) if a or b]
    return sorted(pairs, key=lambda p: -weight(*p))


def encode(v):
    peak = jnp.max(jnp.max(jnp.abs(v), axis=0, keepdims=True), axis=1, keepdims=True)
    peak = jnp.maximum(peak, 1e-30).astype(jnp.bfloat16).astype(F32)
    t = v * (128.0 / peak)
    t4 = (t * t) * (t * t)
    t8 = t4 * t4
    t16 = t8 * t8
    code = jnp.where(v < 0, -t16, t16).astype(jnp.bfloat16)
    return code, jnp.broadcast_to(peak, (SCALE_ROWS, v.shape[1])).astype(jnp.bfloat16)


def decode(code, peak):
    y = code.astype(F32)
    size = jnp.abs(y)
    r = jnp.exp2(jnp.log2(jnp.maximum(size, 1e-37)) * (1.0 / 16.0) - 7.0)
    r = jnp.where(size > 1e-37, r, 0.0) * peak[:1].astype(F32)
    return jnp.where(y < 0, -r, r)


def split(v):
    high = v.astype(jnp.bfloat16)
    return high, (v - high.astype(F32)).astype(jnp.bfloat16)


def dot_split(a, b):
    a_high, a_low = split(a)
    b_high, b_low = split(b)
    k = b.shape[1]
    wide = jnp.dot(a_high, jnp.concatenate([b_high, b_low], axis=1), preferred_element_type=F32)
    return wide[:, :k] + (wide[:, k:] + jnp.dot(a_low, b_high, preferred_element_type=F32))


def cholesky_panels(aug, first, last):
    k = aug.shape[0]

    def panel(p, carry):
        base = pl.multiple_of(p * PANEL, PANEL)
        rows = aug[pl.ds(base, PANEL), :]
        lane = lax.broadcasted_iota(jnp.int32, (PANEL, 2 * k), 1)
        sub = lax.broadcasted_iota(jnp.int32, (PANEL, 1), 0)
        left = rows[:, :k]
        lane_k = lax.broadcasted_iota(jnp.int32, (PANEL, k), 1)
        cols = [
            jnp.sum(jnp.where(lane_k == base + i, left, 0.0), axis=1, keepdims=True)
            for i in range(PANEL)
        ]
        for i in range(PANEL):
            scale = lax.rsqrt(cols[i][i : i + 1, :])
            factor = jnp.where(sub > i, cols[i] * scale, 0.0)
            keep = sub == i
            head = rows[i : i + 1, :] * scale
            rows = jnp.where(keep, head, rows - factor * head)
            for m in range(i + 1, PANEL):
                cols[m] = cols[m] - factor * (cols[m][i : i + 1, :] * scale)
        aug[pl.ds(base, PANEL), :] = rows
        upper = jnp.where(lane_k >= base + PANEL, rows[:, :k], 0.0)
        aug[...] = aug[...] - dot32(upper.T, rows)
        return carry

    lax.fori_loop(first, last, panel, 0)


def body(
    nx, ny, nz, scale,
    grad, act, err, right0, momentum,
    merged, lhat_out, s_full, sown_out, inv_out, momentum_out,
    grad_v, act_all, grad_t, err_v, r_all, m_tile, m_t,
    xt, yt, xr, yr, xs, ys, xf, yf, top, bottom,
    p_plane, r_plane, f_plane, p_col, r_col, f_col, p_gram, r_gram, f_gram, aug,
    local_sem, up_send, up_recv, down_send, down_recv, sib_send, sib_recv,
    rs_send, rs_recv, x_send, x_recv, y_send, y_recv, xf_send, xf_recv, yf_send, yf_recv,
    ps_send, ps_recv, pg_send, pg_recv, cs_send, cs_recv, cg_send, cg_recv, gs_send, gs_recv, gg_send, gg_recv,
    ag_send, ag_recv, dd_send, dd_recv,
):
    d, j = lax.axis_index("dp"), lax.axis_index("rows")
    y, x = d // nx, d % nx
    z, c = j // 2, j % 2
    tok, cb = act.shape
    rb_rows = grad.shape[1]
    half_rows = rb_rows // 2
    n = nx * ny
    far = nz // 2
    th = tok // PARTS

    def plane_id(dy, dx):
        return (((y + dy) % ny) * nx + (x + dx) % nx, j)

    def col_id(dz, dc):
        return (d, ((z + dz) % nz) * 2 + (c + dc) % 2)

    plane = far_first(ny, nx, lambda a, b: ring_dist(a, ny) + ring_dist(b, nx))
    column = far_first(nz, 2, lambda a, b: ring_dist(a, nz) + 0.1 * b)

    def remote(src, dst, send, recv, device):
        return pltpu.make_async_remote_copy(
            src_ref=src, dst_ref=dst, send_sem=send, recv_sem=recv,
            device_id=device, device_id_type=MESH,
        )

    load_act = pltpu.make_async_copy(act, act_all.at[0, 0], local_sem.at[0])
    load_act.start()
    load_grad = pltpu.make_async_copy(grad, grad_v, local_sem.at[3])
    load_grad.start()
    load_err = pltpu.make_async_copy(err.at[0], err_v, local_sem.at[1])
    load_err.start()

    barrier = pltpu.get_barrier_semaphore()
    near = [plane_id(dy, 0) for dy in range(1, ny)] + [plane_id(0, dx) for dx in range(1, nx)]
    near += [col_id(dz, 0) for dz in range(1, nz)] + [col_id(0, 1)]
    for device in near:
        pl.semaphore_signal(barrier, inc=1, device_id=device, device_id_type=MESH)
    sr = rb_rows // n
    gr = aug.shape[0] // n
    k = aug.shape[0]
    load_right = pltpu.make_async_copy(right0.at[pl.ds(pl.multiple_of(d * sr, sr), sr)], r_all.at[x, y, c, z], local_sem.at[2])
    load_right.start()
    load_act.wait()
    load_right.wait()
    pl.semaphore_wait(barrier, len(near))

    pending = []

    def wait_bytes(ref, sem):
        pltpu.make_async_copy(ref, ref, sem).wait()

    far_z = sorted(range(1, nz), key=lambda dz: -ring_dist(dz, nz))

    class Everywhere:
        def __init__(self, buf, which):
            self.buf, self.which = buf, which
            half = nz // 2
            self.q = (pl.ds(0, half), pl.ds(half, nz - half))
            pending.append(self.sent)

        def column_start(self):
            ref = self.buf.at[x, y, c, z]
            for dz in far_z:
                remote(ref, ref, rs_send.at[self.which], rs_recv.at[self.which], col_id(dz, 0)).start()

        def column_wait(self):
            wait_bytes(self.buf.at[x, y, c, pl.ds(0, nz - 1)], rs_recv.at[self.which])

        def move(self, step, delta):
            q = self.q[step % 2]
            at = (x, y) if step < 2 else ((slice(None), y) if step == 2 else (x, slice(None)))
            ref = self.buf.at[at[0], at[1], c, q]
            along_x = step in (0, 3)
            return remote(ref, ref, ag_send.at[self.which, step, delta - 1], ag_recv.at[self.which, step, delta - 1],
                          plane_id(0, delta) if along_x else plane_id(delta, 0))

        def share(self, i):
            if i < ny:
                ref = self.buf.at[:, (y - i + ny) % ny, c, self.q[0]]
            else:
                ref = self.buf.at[(x - (i - ny) + nx) % nx, :, c, self.q[1]]
            return remote(ref, ref, dd_send.at[self.which, i], dd_recv.at[self.which, i], col_id(0, 1))

        def first(self):
            for dx in range(1, nx):
                self.move(0, dx).start()
            for dy in range(1, ny):
                self.move(1, dy).start()

        def second(self):
            for dx in range(1, nx):
                self.move(0, dx).wait_recv()
            for dy in range(1, ny):
                self.move(2, dy).start()
            for dy in range(1, ny):
                self.move(1, dy).wait_recv()
            for dx in range(1, nx):
                self.move(3, dx).start()
            self.share(0).start()
            self.share(ny).start()

        def third(self):
            for i in range(1, max(nx, ny)):
                if i < ny:
                    self.move(2, i).wait_recv()
                    self.share(i).start()
                if i < nx:
                    self.move(3, i).wait_recv()
                    self.share(ny + i).start()

        def last(self):
            for i in range(nx + ny):
                self.share(i).wait_recv()

        def sent(self):
            wait_bytes(self.buf.at[x, y, c, pl.ds(0, nz - 1)], rs_send.at[self.which])
            for step in range(4):
                for delta in range(1, nx if step in (0, 3) else ny):
                    self.move(step, delta).wait_send()
            for i in range(nx + ny):
                self.share(i).wait_send()

    right_in = Everywhere(r_all, 0)
    right_out = Everywhere(s_full, 1)
    right_in.column_start()

    def half(slot, h):
        return act_all.at[slot, 0, pl.ds(h * th, th)]

    def up(s, h):
        return remote(half((nz - s + 1) % nz, h), half(nz - s, h), up_send.at[s - 1, h], up_recv.at[s - 1, h], col_id(1, 0))

    def down(s, h):
        return remote(half(s - 1, h), half(s, h), down_send.at[s - 1, h], down_recv.at[s - 1, h], col_id(nz - 1, 0))

    def sibling(slot, h):
        return remote(half(slot, h), act_all.at[slot, 1, pl.ds(h * th, th)], sib_send.at[slot, h], sib_recv.at[slot, h], col_id(0, 1))

    mid = PARTS // 2
    up_list = [(s, h) for s in range(1, far) for h in range(PARTS)] + [(far, h) for h in range(mid)]
    down_list = [(s, PARTS - 1 - h) for s, h in up_list]

    def gather_sent():
        for s, h in up_list:
            up(s, h).wait_send()
        for s, h in down_list:
            down(s, h).wait_send()
        for slot in range(nz):
            for h in range(PARTS):
                sibling(slot, h).wait_send()

    pending.append(gather_sent)
    for ua, da in zip(up_list[:PARTS], down_list[:PARTS]):
        up(*ua).start()
        down(*da).start()
    for h in range(PARTS):
        sibling(0, h).start()

    load_grad.wait()
    grad_t[...] = grad_v[...].astype(F32).T.astype(jnp.bfloat16)
    load_err.wait()
    load_momentum = pltpu.make_async_copy(momentum, momentum_out, local_sem.at[1])
    load_momentum.start()
    pending.append(load_momentum.wait)
    def block_of(slot, dc):
        return ((z + slot) % nz) * 2 + (c + dc) % 2

    def columns(b):
        return pl.ds(pl.multiple_of(b * cb, cb), cb)

    def x_copy(b, dx, slot=0):
        return remote(xt.at[slot], xr.at[b % ny, dx - 1],
                      x_send.at[slot], x_recv.at[b % ny, dx - 1], plane_id(0, dx))

    def y_copy(b, dy, slot=0):
        return remote(yt.at[slot], yr.at[b // ny, dy - 1],
                      y_send.at[slot], y_recv.at[b // ny, dy - 1], plane_id(dy, 0))

    def put(ref, index, v):
        code, peak = encode(v)
        ref[index, :half_rows] = code
        ref[index, half_rows:] = peak

    def get(ref, *index):
        message = ref[index]
        return decode(message[:half_rows], message[half_rows:])

    def produce(slot, dc):
        cols = columns(block_of(slot, dc))
        merged[:, cols] = jnp.dot(grad_t[...], act_all[slot, dc], preferred_element_type=F32) + err_v[:, cols]

    def send(slot, dc):
        b = block_of(slot, dc)
        owner_x, owner_y = b // ny, b % ny
        at = 2 * slot + dc
        code, peak = encode(merged[:, columns(b)])
        xt[at, :half_rows] = code[:half_rows]
        yt[at, :half_rows] = code[half_rows:]
        xt[at, half_rows:] = peak
        yt[at, half_rows:] = peak
        if nx > 1:
            @pl.when(owner_x != x)
            def _():
                x_copy(b, (owner_x - x + nx) % nx, at).start()
        if ny > 1:
            @pl.when(owner_y != y)
            def _():
                y_copy(b, (owner_y - y + ny) % ny, at).start()

    def xf_copy(dy):
        return remote(xs.at[dy - 1], xf.at[dy - 1], xf_send.at[dy - 1], xf_recv.at[dy - 1], plane_id(dy, 0))

    def yf_copy(dx):
        return remote(ys.at[dx - 1], yf.at[dx - 1], yf_send.at[dx - 1], yf_recv.at[dx - 1], plane_id(0, dx))

    def consume(slot, dc):
        b = block_of(slot, dc)
        cols = columns(b)
        owner_x, owner_y = b // ny, b % ny

        @pl.when(owner_x == x)
        def _():
            total = merged[pl.ds(0, half_rows), cols]
            for dx in range(1, nx):
                x_copy(b, dx).wait_recv()
                total = total + get(xr, b % ny, dx - 1)

            @pl.when(owner_y == y)
            def _():
                top[...] = total

            @pl.when(owner_y != y)
            def _():
                dy = (owner_y - y + ny) % ny
                put(xs, dy - 1, total)
                xf_copy(dy).start()

        @pl.when(owner_y == y)
        def _():
            total = merged[pl.ds(half_rows, half_rows), cols]
            for dy in range(1, ny):
                y_copy(b, dy).wait_recv()
                total = total + get(yr, b // ny, dy - 1)

            @pl.when(owner_x == x)
            def _():
                bottom[...] = total

            @pl.when(owner_x != x)
            def _():
                dx = (owner_x - x + nx) % nx
                put(ys, dx - 1, total)
                yf_copy(dx).start()

    def tiles_sent():
        @pl.loop(0, n)
        def _(at):
            b = block_of(at // 2, at % 2)

            @pl.when(b // ny != x)
            def _():
                x_copy(b, 1, at).wait_send()

            @pl.when(b % ny != y)
            def _():
                y_copy(b, 1, at).wait_send()
        for dy in range(1, ny):
            xf_copy(dy).wait_send()
        for dx in range(1, nx):
            yf_copy(dx).wait_send()

    def multiply(slot, dc):
        b = block_of(slot, dc)
        strips = [r_all[i, h, b % 2, b // 2] for h in range(ny) for i in range(nx)]
        product = dot_split(merged[:, columns(b)], jnp.concatenate(strips, axis=0))
        p_plane[0] = p_plane[0] + (product * scale).reshape(n, sr, k)

    def ring_pair(s, act):
        @pl.loop(0, jnp.where(s == 0, 1, 2))
        def _(t):
            act(jnp.where(t == 0, (nz - s) % nz, s))

    def plane_scatter(stage):
        pending.append(lambda: wait_bytes(r_plane.at[stage], ps_send.at[stage]))
        pending.append(lambda: wait_bytes(r_plane.at[stage], pg_send.at[stage]))
        for i, (dy, dx) in enumerate(plane):
            dev = plane_id(dy, dx)
            remote(p_plane.at[stage, dev[0]], r_plane.at[stage, i], ps_send.at[stage], ps_recv.at[stage], dev).start()

    def plane_gather(stage):
        wait_bytes(r_plane.at[stage], ps_recv.at[stage])
        total = p_plane[stage, d]
        for i in range(len(plane)):
            total = total + r_plane[stage, i]
        f_plane[stage, d] = total
        for dy, dx in plane:
            remote(f_plane.at[stage, d], f_plane.at[stage, d], pg_send.at[stage], pg_recv.at[stage], plane_id(dy, dx)).start()

    def plane_finish(stage):
        wait_bytes(r_plane.at[stage], pg_recv.at[stage])
        return f_plane[stage].reshape(rb_rows, k)

    pending.append(tiles_sent)
    p_plane[0] = jnp.zeros((n, sr, k), F32)
    steps = len(up_list)
    gathered_late = steps <= 12
    produce(0, 0)
    send(0, 0)

    def ring_step(i):
        s, h = i // PARTS + 1, i % PARTS
        more = jnp.logical_or(s + 1 < far, jnp.logical_and(s + 1 == far, h < mid))
        up(s, h).wait_recv()

        @pl.when(more)
        def _():
            up(s + 1, h).start()
        sibling(nz - s, h).start()
        down(s, PARTS - 1 - h).wait_recv()

        @pl.when(more)
        def _():
            down(s + 1, PARTS - 1 - h).start()
        sibling(s, PARTS - 1 - h).start()

    @pl.loop(0, steps - 1)
    def _(i):
        ring_step(i)
        if not gathered_late:
            @pl.when(i == 1)
            def _():
                right_in.column_wait()
                right_in.first()

            @pl.when(i == 5)
            def _():
                right_in.second()

            @pl.when(i == 9)
            def _():
                right_in.third()

            @pl.when(i == 10)
            def _():
                right_in.last()

                @pl.loop(0, 2 * (far - 1))
                def _(t):
                    ring_pair(t // 2, lambda slot: multiply(slot, t % 2))

        @pl.when(jnp.logical_or(i % PARTS == PARTS - 1, i % PARTS == 0))
        def _():
            s, dc = (i + 1) // PARTS, jnp.where(i % PARTS == 0, 1, 0)

            @pl.when(dc == 1)
            def _():
                def landed(slot):
                    for h in range(PARTS):
                        sibling(slot, h).wait_recv()
                ring_pair(s, landed)

            def fresh(slot):
                produce(slot, dc)
                send(slot, dc)
            ring_pair(s, fresh)

            @pl.when(s > 0)
            def _():
                ring_pair(s - 1, lambda slot: consume(slot, dc))

    ring_step(steps - 1)
    if gathered_late:
        right_in.column_wait()
        right_in.first()
        right_in.second()
        right_in.third()
        right_in.last()

        @pl.loop(0, 2 * (far - 1))
        def _(t):
            ring_pair(t // 2, lambda slot: multiply(slot, t % 2))

    @pl.loop(0, 2)
    def _(dc):
        ring_pair(far - 1, lambda slot: multiply(slot, dc))
    for h in range(PARTS):
        sibling(far, h).wait_recv()

    @pl.loop(0, 2)
    def _(dc):
        produce(far, dc)
        multiply(far, dc)
    plane_scatter(0)

    @pl.loop(0, 2)
    def _(dc):
        send(far, dc)

    @pl.loop(0, 2)
    def _(dc):
        ring_pair(far - 1, lambda slot: consume(slot, dc))
    plane_gather(0)

    @pl.loop(0, 2)
    def _(dc):
        consume(far, dc)

    acc = top[...]
    for dy in range(1, ny):
        xf_copy(dy).wait_recv()
        acc = acc + get(xf, dy - 1)
    m_tile[pl.ds(0, half_rows), :] = acc * scale
    acc = bottom[...]
    for dx in range(1, nx):
        yf_copy(dx).wait_recv()
        acc = acc + get(yf, dx - 1)
    m_tile[pl.ds(half_rows, half_rows), :] = acc * scale

    factor_col = (p_col, r_col, f_col, cs_send, cs_recv, cg_send, cg_recv)
    gram_col = (p_gram, r_gram, f_gram, gs_send, gs_recv, gg_send, gg_recv)

    def col_scatter(stage, what, both=True):
        part, got, full, s_send, s_recv, g_send, g_recv = what
        pending.append(lambda: wait_bytes(got.at[stage], s_send.at[stage]))
        if both:
            pending.append(lambda: wait_bytes(got.at[stage], g_send.at[stage]))
        for i, (dz, dc) in enumerate(column):
            dev = col_id(dz, dc)
            remote(part.at[stage, dev[1]], got.at[stage, i], s_send.at[stage], s_recv.at[stage], dev).start()

    def col_total(stage, what):
        part, got, full, s_send, s_recv, g_send, g_recv = what
        wait_bytes(got.at[stage], s_recv.at[stage])
        total = part[stage, j]
        for i in range(len(column)):
            total = total + got[stage, i]
        return total

    def col_gather(stage, what):
        part, got, full, s_send, s_recv, g_send, g_recv = what
        full[stage, j] = col_total(stage, what)
        for dz, dc in column:
            remote(full.at[stage, j], full.at[stage, j], g_send.at[stage], g_recv.at[stage], col_id(dz, dc)).start()

    def col_finish(stage, what):
        part, got, full, s_send, s_recv, g_send, g_recv = what
        wait_bytes(got.at[stage], g_recv.at[stage])
        return full[stage].reshape(-1, k)

    def right_of(stage, left):
        p_col[stage] = dot_split(m_t[...], left).reshape(n, sr, k)
        col_scatter(stage, factor_col, stage == 0)
        p_gram[stage] = dot32(left, left, ((0,), (0,))).reshape(n, gr, k)
        col_scatter(stage, gram_col)
        if stage == 0:
            col_gather(stage, factor_col)
        else:
            s_full[x, y, c, z] = col_total(stage, factor_col)
            right_out.column_start()
        col_gather(stage, gram_col)

    def set_aug(gram):
        row = lax.broadcasted_iota(jnp.int32, (k, k), 0)
        col = lax.broadcasted_iota(jnp.int32, (k, k), 1)
        aug[:, :k] = gram
        aug[:, k:] = jnp.where(row == col, 1.0, 0.0).astype(F32)

    panels = k // PANEL

    m_t[...] = m_tile[...].T
    left = plane_finish(0)
    right_of(0, left)
    s_one = col_finish(0, factor_col)
    p_plane[1] = dot_split(m_tile[...], s_one).reshape(n, sr, k)
    plane_scatter(1)
    set_aug(col_finish(0, gram_col))
    cholesky_panels(aug, 0, panels // 2)
    plane_gather(1)
    cholesky_panels(aug, panels // 2, panels)
    left = dot32(plane_finish(1), aug[:, k:], ((1,), (1,)))
    right_of(1, left)

    right_out.column_wait()
    right_out.first()
    set_aug(col_finish(1, gram_col))
    cholesky_panels(aug, 0, panels // 2)
    right_out.second()
    cholesky_panels(aug, panels // 2, panels)
    inverse = aug[:, k:]
    inv_out[...] = inverse
    lhat_out[...] = dot32(dot32(left, inverse, ((1,), (1,))), inverse)
    right_out.third()
    right_out.last()
    sown_out[...] = ordered(s_full, j // ny, j % ny)

    for wait in pending:
        wait()


def ordered(ref, *index):
    cores, depth = ref.shape[-4], ref.shape[-3]
    return jnp.concatenate([ref[(*index, c, z)] for z in range(depth) for c in range(cores)], axis=0)


def rows_of(ref):
    return ref.shape[1] * ref.shape[2] * ref.shape[3]


def finish_body(wide, merged, lhat, s, momentum, sown, inverse, error, new_momentum, right, e_buf, m_buf, sem):
    total = merged.shape[1]
    l_high, l_low = split(lhat[...])
    l_all = jnp.concatenate([l_high, l_high, l_low], axis=1)

    def copies(i):
        cols = pl.ds(i * wide, wide)
        return (
            pltpu.make_async_copy(e_buf.at[i], error.at[0, :, cols], sem.at[i, 0]),
            pltpu.make_async_copy(m_buf.at[i], new_momentum.at[:, cols], sem.at[i, 1]),
        )

    for i in range(total // wide):
        cols = pl.ds(i * wide, wide)
        blocks = wide // rows_of(s)
        s_high, s_low = split(jnp.concatenate([ordered(s, i * blocks + h) for h in range(blocks)], axis=0))
        s_all = jnp.concatenate([s_high, s_low, s_high], axis=1)
        approx = lax.dot_general(l_all, s_all, (((1,), (1,)), ((), ())), preferred_element_type=F32)
        e_buf[i] = merged[:, cols] - approx
        m_buf[i] = (MOMENTUM_RATE * momentum[:, cols].astype(F32) + approx).astype(jnp.bfloat16)
        for copy in copies(i):
            copy.start()
    right[...] = dot32(sown[...], inverse[...], ((1,), (1,)))
    for i in range(total // wide):
        for copy in copies(i):
            copy.wait()


def per_device(nx, ny, nz, grad_out, activations, error_feedback, momentum, right_factor):
    n = nx * ny
    tok, cb = activations.shape
    rows = grad_out.shape[1]
    total = error_feedback.shape[2]
    k = right_factor.shape[1]
    sr, gr, hr = rows // n, k // n, rows // 2
    far = nz // 2
    vmem, dma = pltpu.VMEM, pltpu.SemaphoreType.DMA
    scratch = [
        vmem((tok, rows), jnp.bfloat16),
        vmem((nz, 2, tok, cb), jnp.bfloat16),
        vmem((rows, tok), jnp.bfloat16),
        vmem((rows, total), F32),
        vmem((nx, ny, 2, nz, sr, k), F32),
        vmem((rows, cb), F32),
        vmem((cb, rows), F32),
        vmem((n, hr + SCALE_ROWS, cb), jnp.bfloat16),
        vmem((n, hr + SCALE_ROWS, cb), jnp.bfloat16),
        vmem((ny, max(nx - 1, 1), hr + SCALE_ROWS, cb), jnp.bfloat16),
        vmem((nx, max(ny - 1, 1), hr + SCALE_ROWS, cb), jnp.bfloat16),
        vmem((max(ny - 1, 1), hr + SCALE_ROWS, cb), jnp.bfloat16),
        vmem((max(nx - 1, 1), hr + SCALE_ROWS, cb), jnp.bfloat16),
        vmem((max(ny - 1, 1), hr + SCALE_ROWS, cb), jnp.bfloat16),
        vmem((max(nx - 1, 1), hr + SCALE_ROWS, cb), jnp.bfloat16),
        vmem((hr, cb), F32),
        vmem((hr, cb), F32),
        vmem((2, n, sr, k), F32),
        vmem((2, n - 1, sr, k), F32),
        vmem((2, n, sr, k), F32),
        vmem((2, n, sr, k), F32),
        vmem((2, n - 1, sr, k), F32),
        vmem((2, n, sr, k), F32),
        vmem((2, n, gr, k), F32),
        vmem((2, n - 1, gr, k), F32),
        vmem((2, n, gr, k), F32),
        vmem((k, 2 * k), F32),
        dma((4,)),
        dma((far, PARTS)), dma((far, PARTS)), dma((far, PARTS)), dma((far, PARTS)),
        dma((nz, PARTS)), dma((nz, PARTS)),
        dma((2,)), dma((2,)),
        dma((n,)), dma((ny, max(nx - 1, 1))),
        dma((n,)), dma((nx, max(ny - 1, 1))),
        dma((max(ny - 1, 1),)), dma((max(ny - 1, 1),)),
        dma((max(nx - 1, 1),)), dma((max(nx - 1, 1),)),
        dma((2,)), dma((2,)), dma((2,)), dma((2,)),
        dma((2,)), dma((2,)), dma((2,)), dma((2,)),
        dma((2,)), dma((2,)), dma((2,)), dma((2,)),
        dma((2, 4, max(nx, ny))), dma((2, 4, max(nx, ny))),
        dma((2, nx + ny)), dma((2, nx + ny)),
    ]
    any_space = pl.BlockSpec(memory_space=pl.ANY)
    in_vmem = pl.BlockSpec(memory_space=pltpu.VMEM)
    merged, lhat, s, sown, inverse, momentum = pl.pallas_call(
        functools.partial(body, nx, ny, nz, 1.0 / n),
        out_shape=(
            jax.ShapeDtypeStruct((rows, total), F32),
            jax.ShapeDtypeStruct((rows, k), F32),
            jax.ShapeDtypeStruct((nx, ny, 2, nz, sr, k), F32),
            jax.ShapeDtypeStruct((cb, k), F32),
            jax.ShapeDtypeStruct((k, k), F32),
            jax.ShapeDtypeStruct((rows, total), momentum.dtype),
        ),
        in_specs=[any_space] * 5,
        out_specs=(in_vmem,) * 6,
        scratch_shapes=scratch,
        compiler_params=pltpu.CompilerParams(
            collective_id=0, has_side_effects=True, vmem_limit_bytes=VMEM_LIMIT
        ),
        name="compress",
    )(*[pltpu.with_memory_space_constraint(v, pltpu.HBM) for v in (grad_out, activations, error_feedback, right_factor, momentum)])
    s = s.reshape(n, 2, nz, sr, k)
    wide = min(512, total)
    return pl.pallas_call(
        functools.partial(finish_body, wide),
        out_shape=(
            jax.ShapeDtypeStruct((1, rows, total), F32),
            jax.ShapeDtypeStruct((rows, total), jnp.bfloat16),
            jax.ShapeDtypeStruct((cb, k), F32),
        ),
        in_specs=[in_vmem] * 6,
        out_specs=(any_space, any_space, in_vmem),
        scratch_shapes=[
            vmem((total // wide, rows, wide), F32),
            vmem((total // wide, rows, wide), jnp.bfloat16),
            dma((total // wide, 2)),
        ],
        compiler_params=pltpu.CompilerParams(vmem_limit_bytes=20 << 20),
        name="finish",
    )(merged, lhat, s, momentum, sown, inverse)


def build(mesh, nx, ny, nz):
    return jax.shard_map(
        functools.partial(per_device, nx, ny, nz),
        mesh=mesh,
        in_specs=(
            P("dp", "rows"),
            P("dp", "rows"),
            P("dp", "rows", None),
            P("rows", None),
            P("rows", None),
        ),
        out_specs=(P("dp", "rows", None), P("rows", None), P("rows", None)),
        check_vma=False,
    )


def solution(mesh):
    return build(mesh, 4, 4, 8)
```

```python
import functools

import jax
import jax.numpy as jnp
from jax import lax
from jax.experimental import pallas as pl
from jax.experimental.pallas import tpu as pltpu
from jax.sharding import PartitionSpec as P

MOMENTUM_RATE = 0.9
HIGHEST = lax.Precision.HIGHEST
MESH = pl.DeviceIdType.MESH
F32 = jnp.float32
PANEL = 16
SCALE_ROWS = 16
LAG = 5
PARTS = 4
VMEM_LIMIT = 33_554_432


def dot32(a, b, dims=((1,), (0,))):
    return lax.dot_general(
        a, b, (dims, ((), ())), precision=HIGHEST, preferred_element_type=F32
    )


def ring_dist(delta, size):
    return min(delta, size - delta)


def far_first(n_a, n_b, weight):
    pairs = [(a, b) for a in range(n_a) for b in range(n_b) if a or b]
    return sorted(pairs, key=lambda p: -weight(*p))


def encode(v):
    peak = jnp.max(jnp.max(jnp.abs(v), axis=0, keepdims=True), axis=1, keepdims=True)
    peak = jnp.maximum(peak, 1e-30).astype(jnp.bfloat16).astype(F32)
    t = v * (128.0 / peak)
    t4 = (t * t) * (t * t)
    t8 = t4 * t4
    t16 = t8 * t8
    code = jnp.where(v < 0, -t16, t16).astype(jnp.bfloat16)
    return code, jnp.broadcast_to(peak, (SCALE_ROWS, v.shape[1])).astype(jnp.bfloat16)


def decode(code, peak):
    y = code.astype(F32)
    size = jnp.abs(y)
    r = jnp.exp2(jnp.log2(jnp.maximum(size, 1e-37)) * (1.0 / 16.0) - 7.0)
    r = jnp.where(size > 1e-37, r, 0.0) * peak[:1].astype(F32)
    return jnp.where(y < 0, -r, r)


def split(v):
    high = v.astype(jnp.bfloat16)
    return high, (v - high.astype(F32)).astype(jnp.bfloat16)


def dot_split(a, b):
    a_high, a_low = split(a)
    b_high, b_low = split(b)
    k = b.shape[1]
    wide = jnp.dot(a_high, jnp.concatenate([b_high, b_low], axis=1), preferred_element_type=F32)
    return wide[:, :k] + (wide[:, k:] + jnp.dot(a_low, b_high, preferred_element_type=F32))


def cholesky_panels(aug, first, last):
    k = aug.shape[0]

    def panel(p, carry):
        base = pl.multiple_of(p * PANEL, PANEL)
        rows = aug[pl.ds(base, PANEL), :]
        lane = lax.broadcasted_iota(jnp.int32, (PANEL, 2 * k), 1)
        sub = lax.broadcasted_iota(jnp.int32, (PANEL, 1), 0)
        left = rows[:, :k]
        lane_k = lax.broadcasted_iota(jnp.int32, (PANEL, k), 1)
        cols = [
            jnp.sum(jnp.where(lane_k == base + i, left, 0.0), axis=1, keepdims=True)
            for i in range(PANEL)
        ]
        for i in range(PANEL):
            scale = lax.rsqrt(cols[i][i : i + 1, :])
            factor = jnp.where(sub > i, cols[i] * scale, 0.0)
            keep = sub == i
            head = rows[i : i + 1, :] * scale
            rows = jnp.where(keep, head, rows - factor * head)
            for m in range(i + 1, PANEL):
                cols[m] = cols[m] - factor * (cols[m][i : i + 1, :] * scale)
        aug[pl.ds(base, PANEL), :] = rows
        upper = jnp.where(lane_k >= base + PANEL, rows[:, :k], 0.0)
        aug[...] = aug[...] - dot32(upper.T, rows)
        return carry

    lax.fori_loop(first, last, panel, 0)


def body(
    nx, ny, nz, scale,
    grad, act, err, right0, momentum,
    merged, lhat_out, s_full, sown_out, inv_out, momentum_out,
    grad_v, act_all, grad_t, err_v, r_all, m_tile, m_t,
    xt, yt, xr, yr, xs, ys, xf, yf, top, bottom,
    p_plane, r_plane, f_plane, p_col, r_col, f_col, p_gram, r_gram, f_gram, aug,
    local_sem, up_send, up_recv, down_send, down_recv, sib_send, sib_recv,
    rs_send, rs_recv, x_send, x_recv, y_send, y_recv, xf_send, xf_recv, yf_send, yf_recv,
    ps_send, ps_recv, pg_send, pg_recv, cs_send, cs_recv, cg_send, cg_recv, gs_send, gs_recv, gg_send, gg_recv,
    ag_send, ag_recv, dd_send, dd_recv,
):
    d, j = lax.axis_index("dp"), lax.axis_index("rows")
    y, x = d // nx, d % nx
    z, c = j // 2, j % 2
    tok, cb = act.shape
    rb_rows = grad.shape[1]
    half_rows = rb_rows // 2
    n = nx * ny
    far = nz // 2
    th = tok // PARTS

    def plane_id(dy, dx):
        return (((y + dy) % ny) * nx + (x + dx) % nx, j)

    def col_id(dz, dc):
        return (d, ((z + dz) % nz) * 2 + (c + dc) % 2)

    plane = far_first(ny, nx, lambda a, b: ring_dist(a, ny) + ring_dist(b, nx))
    column = far_first(nz, 2, lambda a, b: ring_dist(a, nz) + 0.1 * b)

    def remote(src, dst, send, recv, device):
        return pltpu.make_async_remote_copy(
            src_ref=src, dst_ref=dst, send_sem=send, recv_sem=recv,
            device_id=device, device_id_type=MESH,
        )

    load_act = pltpu.make_async_copy(act, act_all.at[0, 0], local_sem.at[0])
    load_act.start()
    load_grad = pltpu.make_async_copy(grad, grad_v, local_sem.at[3])
    load_grad.start()
    load_err = pltpu.make_async_copy(err.at[0], err_v, local_sem.at[1])
    load_err.start()

    barrier = pltpu.get_barrier_semaphore()
    near = [plane_id(dy, 0) for dy in range(1, ny)] + [plane_id(0, dx) for dx in range(1, nx)]
    near += [col_id(dz, 0) for dz in range(1, nz)] + [col_id(0, 1)]
    for device in near:
        pl.semaphore_signal(barrier, inc=1, device_id=device, device_id_type=MESH)
    sr = rb_rows // n
    gr = aug.shape[0] // n
    k = aug.shape[0]
    load_right = pltpu.make_async_copy(right0.at[pl.ds(pl.multiple_of(d * sr, sr), sr)], r_all.at[x, y, c, z], local_sem.at[2])
    load_right.start()
    load_act.wait()
    load_right.wait()
    pl.semaphore_wait(barrier, len(near))

    pending = []

    def wait_bytes(ref, sem):
        pltpu.make_async_copy(ref, ref, sem).wait()

    far_z = sorted(range(1, nz), key=lambda dz: -ring_dist(dz, nz))

    class Everywhere:
        def __init__(self, buf, which):
            self.buf, self.which = buf, which
            half = nz // 2
            self.q = (pl.ds(0, half), pl.ds(half, nz - half))
            pending.append(self.sent)

        def column_start(self):
            ref = self.buf.at[x, y, c, z]
            for dz in far_z:
                remote(ref, ref, rs_send.at[self.which], rs_recv.at[self.which], col_id(dz, 0)).start()

        def column_wait(self):
            wait_bytes(self.buf.at[x, y, c, pl.ds(0, nz - 1)], rs_recv.at[self.which])

        def move(self, step, delta):
            q = self.q[step % 2]
            at = (x, y) if step < 2 else ((slice(None), y) if step == 2 else (x, slice(None)))
            ref = self.buf.at[at[0], at[1], c, q]
            along_x = step in (0, 3)
            return remote(ref, ref, ag_send.at[self.which, step, delta - 1], ag_recv.at[self.which, step, delta - 1],
                          plane_id(0, delta) if along_x else plane_id(delta, 0))

        def share(self, i):
            if i < ny:
                ref = self.buf.at[:, (y - i + ny) % ny, c, self.q[0]]
            else:
                ref = self.buf.at[(x - (i - ny) + nx) % nx, :, c, self.q[1]]
            return remote(ref, ref, dd_send.at[self.which, i], dd_recv.at[self.which, i], col_id(0, 1))

        def first(self):
            for dx in range(1, nx):
                self.move(0, dx).start()
            for dy in range(1, ny):
                self.move(1, dy).start()

        def second(self):
            for dx in range(1, nx):
                self.move(0, dx).wait_recv()
            for dy in range(1, ny):
                self.move(2, dy).start()
            for dy in range(1, ny):
                self.move(1, dy).wait_recv()
            for dx in range(1, nx):
                self.move(3, dx).start()
            self.share(0).start()
            self.share(ny).start()

        def third(self):
            for i in range(1, max(nx, ny)):
                if i < ny:
                    self.move(2, i).wait_recv()
                    self.share(i).start()
                if i < nx:
                    self.move(3, i).wait_recv()
                    self.share(ny + i).start()

        def last(self):
            for i in range(nx + ny):
                self.share(i).wait_recv()

        def sent(self):
            wait_bytes(self.buf.at[x, y, c, pl.ds(0, nz - 1)], rs_send.at[self.which])
            for step in range(4):
                for delta in range(1, nx if step in (0, 3) else ny):
                    self.move(step, delta).wait_send()
            for i in range(nx + ny):
                self.share(i).wait_send()

    right_in = Everywhere(r_all, 0)
    right_out = Everywhere(s_full, 1)
    right_in.column_start()

    def half(slot, h):
        return act_all.at[slot, 0, pl.ds(h * th, th)]

    def up(s, h):
        return remote(half((nz - s + 1) % nz, h), half(nz - s, h), up_send.at[s - 1, h], up_recv.at[s - 1, h], col_id(1, 0))

    def down(s, h):
        return remote(half(s - 1, h), half(s, h), down_send.at[s - 1, h], down_recv.at[s - 1, h], col_id(nz - 1, 0))

    def sibling(slot, h):
        return remote(half(slot, h), act_all.at[slot, 1, pl.ds(h * th, th)], sib_send.at[slot, h], sib_recv.at[slot, h], col_id(0, 1))

    mid = PARTS // 2
    up_list = [(s, h) for s in range(1, far) for h in range(PARTS)] + [(far, h) for h in range(mid)]
    down_list = [(s, PARTS - 1 - h) for s, h in up_list]

    def gather_sent():
        for s, h in up_list:
            up(s, h).wait_send()
        for s, h in down_list:
            down(s, h).wait_send()
        for slot in range(nz):
            for h in range(PARTS):
                sibling(slot, h).wait_send()

    pending.append(gather_sent)
    for ua, da in zip(up_list[:PARTS], down_list[:PARTS]):
        up(*ua).start()
        down(*da).start()
    for h in range(PARTS):
        sibling(0, h).start()

    load_grad.wait()
    grad_t[...] = grad_v[...].astype(F32).T.astype(jnp.bfloat16)
    load_err.wait()
    load_momentum = pltpu.make_async_copy(momentum, momentum_out, local_sem.at[1])
    load_momentum.start()
    pending.append(load_momentum.wait)
    def block_of(slot, dc):
        return ((z + slot) % nz) * 2 + (c + dc) % 2

    def columns(b):
        return pl.ds(pl.multiple_of(b * cb, cb), cb)

    def x_copy(b, dx, slot=0):
        return remote(xt.at[slot], xr.at[b % ny, dx - 1],
                      x_send.at[slot], x_recv.at[b % ny, dx - 1], plane_id(0, dx))

    def y_copy(b, dy, slot=0):
        return remote(yt.at[slot], yr.at[b // ny, dy - 1],
                      y_send.at[slot], y_recv.at[b // ny, dy - 1], plane_id(dy, 0))

    def put(ref, index, v):
        code, peak = encode(v)
        ref[index, :half_rows] = code
        ref[index, half_rows:] = peak

    def get(ref, *index):
        message = ref[index]
        return decode(message[:half_rows], message[half_rows:])

    def produce(slot, dc):
        if dc == 1:
            for h in range(PARTS):
                sibling(slot, h).wait_recv()
        cols = columns(block_of(slot, dc))
        merged[:, cols] = jnp.dot(grad_t[...], act_all[slot, dc], preferred_element_type=F32) + err_v[:, cols]

    def send(slot, dc):
        b = block_of(slot, dc)
        owner_x, owner_y = b // ny, b % ny
        at = 2 * slot + dc
        code, peak = encode(merged[:, columns(b)])
        xt[at, :half_rows] = code[:half_rows]
        yt[at, :half_rows] = code[half_rows:]
        xt[at, half_rows:] = peak
        yt[at, half_rows:] = peak
        if nx > 1:
            @pl.when(owner_x != x)
            def _():
                x_copy(b, (owner_x - x + nx) % nx, at).start()
        if ny > 1:
            @pl.when(owner_y != y)
            def _():
                y_copy(b, (owner_y - y + ny) % ny, at).start()

    def xf_copy(dy):
        return remote(xs.at[dy - 1], xf.at[dy - 1], xf_send.at[dy - 1], xf_recv.at[dy - 1], plane_id(dy, 0))

    def yf_copy(dx):
        return remote(ys.at[dx - 1], yf.at[dx - 1], yf_send.at[dx - 1], yf_recv.at[dx - 1], plane_id(0, dx))

    def consume(slot, dc):
        b = block_of(slot, dc)
        cols = columns(b)
        owner_x, owner_y = b // ny, b % ny

        @pl.when(owner_x == x)
        def _():
            total = merged[pl.ds(0, half_rows), cols]
            for dx in range(1, nx):
                x_copy(b, dx).wait_recv()
                total = total + get(xr, b % ny, dx - 1)

            @pl.when(owner_y == y)
            def _():
                top[...] = total

            @pl.when(owner_y != y)
            def _():
                dy = (owner_y - y + ny) % ny
                put(xs, dy - 1, total)
                xf_copy(dy).start()

        @pl.when(owner_y == y)
        def _():
            total = merged[pl.ds(half_rows, half_rows), cols]
            for dy in range(1, ny):
                y_copy(b, dy).wait_recv()
                total = total + get(yr, b // ny, dy - 1)

            @pl.when(owner_x == x)
            def _():
                bottom[...] = total

            @pl.when(owner_x != x)
            def _():
                dx = (owner_x - x + nx) % nx
                put(ys, dx - 1, total)
                yf_copy(dx).start()

    def tiles_sent():
        for slot in range(nz):
            for dc in (0, 1):
                b, at = block_of(slot, dc), 2 * slot + dc

                @pl.when(b // ny != x)
                def _(b=b, at=at):
                    x_copy(b, 1, at).wait_send()

                @pl.when(b % ny != y)
                def _(b=b, at=at):
                    y_copy(b, 1, at).wait_send()
        for dy in range(1, ny):
            xf_copy(dy).wait_send()
        for dx in range(1, nx):
            yf_copy(dx).wait_send()

    def multiply(pairs):
        total = jnp.zeros((rb_rows, k), F32)
        for slot, dc in pairs:
            b = block_of(slot, dc)
            strips = [r_all[i, h, b % 2, b // 2] for h in range(ny) for i in range(nx)]
            total = total + dot_split(merged[:, columns(b)], jnp.concatenate(strips, axis=0))
        return total

    def plane_scatter(stage):
        pending.append(lambda: wait_bytes(r_plane.at[stage], ps_send.at[stage]))
        pending.append(lambda: wait_bytes(r_plane.at[stage], pg_send.at[stage]))
        for i, (dy, dx) in enumerate(plane):
            dev = plane_id(dy, dx)
            remote(p_plane.at[stage, dev[0]], r_plane.at[stage, i], ps_send.at[stage], ps_recv.at[stage], dev).start()

    def plane_gather(stage):
        wait_bytes(r_plane.at[stage], ps_recv.at[stage])
        total = p_plane[stage, d]
        for i in range(len(plane)):
            total = total + r_plane[stage, i]
        f_plane[stage, d] = total
        for dy, dx in plane:
            remote(f_plane.at[stage, d], f_plane.at[stage, d], pg_send.at[stage], pg_recv.at[stage], plane_id(dy, dx)).start()

    def plane_finish(stage):
        wait_bytes(r_plane.at[stage], pg_recv.at[stage])
        return f_plane[stage].reshape(rb_rows, k)

    pending.append(tiles_sent)
    produce(0, 0)
    send(0, 0)
    later = [[] for _ in range(len(up_list) + 1)]
    later[0].append((0, 1))
    for i, (s, h) in enumerate(up_list):
        if s < far and h == PARTS - 1:
            later[i] += [(nz - s, 0), (s, 0)]
            later[i + 1] += [(nz - s, 1), (s, 1)]
    later[len(up_list) - 1] += [(far, 0), (far, 1)]
    waiting = [[(0, 0)]]
    steps = len(up_list)
    multiplied = []
    for i, ((s, h), (t, g)) in enumerate(zip(up_list, down_list)):
        up(s, h).wait_recv()
        if s + 1 < far or (s + 1 == far and h < mid):
            up(s + 1, h).start()
        sibling(nz - s, h).start()
        down(t, g).wait_recv()
        if t + 1 < far or (t + 1 == far and g >= mid):
            down(t + 1, g).start()
        sibling(t, g).start()
        if i == min(2, steps - 1):
            right_in.column_wait()
            right_in.first()
        if i == min(5, steps - 1):
            right_in.second()
        if i == min(10, steps - 1):
            right_in.third()
        for slot, dc in later[i]:
            produce(slot, dc)
        if i < steps - 1:
            for slot, dc in later[i]:
                send(slot, dc)
        waiting.append(later[i])
        if i < steps - 1 and len(waiting) > LAG:
            for slot, dc in waiting.pop(0):
                consume(slot, dc)
        if i == max(steps - 3, min(10, steps - 1)):
            right_in.last()
            multiplied = [(0, 0)] + [pair for group in later[: i + 1] for pair in group]
            left_sum = multiply(multiplied)
    rest = [pair for group in later for pair in group if pair not in multiplied]
    p_plane[0] = ((left_sum + multiply(rest)) * scale).reshape(n, sr, k)
    plane_scatter(0)
    for slot, dc in later[steps - 1]:
        send(slot, dc)
    for group in waiting[:-1]:
        for slot, dc in group:
            consume(slot, dc)
    plane_gather(0)
    for slot, dc in waiting[-1]:
        consume(slot, dc)

    acc = top[...]
    for dy in range(1, ny):
        xf_copy(dy).wait_recv()
        acc = acc + get(xf, dy - 1)
    m_tile[pl.ds(0, half_rows), :] = acc * scale
    acc = bottom[...]
    for dx in range(1, nx):
        yf_copy(dx).wait_recv()
        acc = acc + get(yf, dx - 1)
    m_tile[pl.ds(half_rows, half_rows), :] = acc * scale

    factor_col = (p_col, r_col, f_col, cs_send, cs_recv, cg_send, cg_recv)
    gram_col = (p_gram, r_gram, f_gram, gs_send, gs_recv, gg_send, gg_recv)

    def col_scatter(stage, what, both=True):
        part, got, full, s_send, s_recv, g_send, g_recv = what
        pending.append(lambda: wait_bytes(got.at[stage], s_send.at[stage]))
        if both:
            pending.append(lambda: wait_bytes(got.at[stage], g_send.at[stage]))
        for i, (dz, dc) in enumerate(column):
            dev = col_id(dz, dc)
            remote(part.at[stage, dev[1]], got.at[stage, i], s_send.at[stage], s_recv.at[stage], dev).start()

    def col_total(stage, what):
        part, got, full, s_send, s_recv, g_send, g_recv = what
        wait_bytes(got.at[stage], s_recv.at[stage])
        total = part[stage, j]
        for i in range(len(column)):
            total = total + got[stage, i]
        return total

    def col_gather(stage, what):
        part, got, full, s_send, s_recv, g_send, g_recv = what
        full[stage, j] = col_total(stage, what)
        for dz, dc in column:
            remote(full.at[stage, j], full.at[stage, j], g_send.at[stage], g_recv.at[stage], col_id(dz, dc)).start()

    def col_finish(stage, what):
        part, got, full, s_send, s_recv, g_send, g_recv = what
        wait_bytes(got.at[stage], g_recv.at[stage])
        return full[stage].reshape(-1, k)

    def right_of(stage, left):
        p_col[stage] = dot_split(m_t[...], left).reshape(n, sr, k)
        col_scatter(stage, factor_col, stage == 0)
        p_gram[stage] = dot32(left, left, ((0,), (0,))).reshape(n, gr, k)
        col_scatter(stage, gram_col)
        if stage == 0:
            col_gather(stage, factor_col)
        else:
            s_full[x, y, c, z] = col_total(stage, factor_col)
            right_out.column_start()
        col_gather(stage, gram_col)

    def set_aug(gram):
        row = lax.broadcasted_iota(jnp.int32, (k, k), 0)
        col = lax.broadcasted_iota(jnp.int32, (k, k), 1)
        aug[:, :k] = gram
        aug[:, k:] = jnp.where(row == col, 1.0, 0.0).astype(F32)

    panels = k // PANEL

    m_t[...] = m_tile[...].T
    left = plane_finish(0)
    right_of(0, left)
    s_one = col_finish(0, factor_col)
    p_plane[1] = dot_split(m_tile[...], s_one).reshape(n, sr, k)
    plane_scatter(1)
    set_aug(col_finish(0, gram_col))
    cholesky_panels(aug, 0, panels // 2)
    plane_gather(1)
    cholesky_panels(aug, panels // 2, panels)
    left = dot32(plane_finish(1), aug[:, k:], ((1,), (1,)))
    right_of(1, left)

    right_out.column_wait()
    right_out.first()
    set_aug(col_finish(1, gram_col))
    cholesky_panels(aug, 0, panels // 2)
    right_out.second()
    cholesky_panels(aug, panels // 2, panels)
    inverse = aug[:, k:]
    inv_out[...] = inverse
    lhat_out[...] = dot32(dot32(left, inverse, ((1,), (1,))), inverse)
    right_out.third()
    right_out.last()
    sown_out[...] = ordered(s_full, j // ny, j % ny)

    for wait in pending:
        wait()


def ordered(ref, *index):
    cores, depth = ref.shape[-4], ref.shape[-3]
    return jnp.concatenate([ref[(*index, c, z)] for z in range(depth) for c in range(cores)], axis=0)


def rows_of(ref):
    return ref.shape[1] * ref.shape[2] * ref.shape[3]


def finish_body(wide, merged, lhat, s, momentum, sown, inverse, error, new_momentum, right, e_buf, m_buf, sem):
    total = merged.shape[1]
    l_high, l_low = split(lhat[...])
    l_all = jnp.concatenate([l_high, l_high, l_low], axis=1)

    def copies(i):
        cols = pl.ds(i * wide, wide)
        return (
            pltpu.make_async_copy(e_buf.at[i], error.at[0, :, cols], sem.at[i, 0]),
            pltpu.make_async_copy(m_buf.at[i], new_momentum.at[:, cols], sem.at[i, 1]),
        )

    for i in range(total // wide):
        cols = pl.ds(i * wide, wide)
        blocks = wide // rows_of(s)
        s_high, s_low = split(jnp.concatenate([ordered(s, i * blocks + h) for h in range(blocks)], axis=0))
        s_all = jnp.concatenate([s_high, s_low, s_high], axis=1)
        approx = lax.dot_general(l_all, s_all, (((1,), (1,)), ((), ())), preferred_element_type=F32)
        e_buf[i] = merged[:, cols] - approx
        m_buf[i] = (MOMENTUM_RATE * momentum[:, cols].astype(F32) + approx).astype(jnp.bfloat16)
        for copy in copies(i):
            copy.start()
    right[...] = dot32(sown[...], inverse[...], ((1,), (1,)))
    for i in range(total // wide):
        for copy in copies(i):
            copy.wait()


def per_device(nx, ny, nz, grad_out, activations, error_feedback, momentum, right_factor):
    n = nx * ny
    tok, cb = activations.shape
    rows = grad_out.shape[1]
    total = error_feedback.shape[2]
    k = right_factor.shape[1]
    sr, gr, hr = rows // n, k // n, rows // 2
    far = nz // 2
    vmem, dma = pltpu.VMEM, pltpu.SemaphoreType.DMA
    scratch = [
        vmem((tok, rows), jnp.bfloat16),
        vmem((nz, 2, tok, cb), jnp.bfloat16),
        vmem((rows, tok), jnp.bfloat16),
        vmem((rows, total), F32),
        vmem((nx, ny, 2, nz, sr, k), F32),
        vmem((rows, cb), F32),
        vmem((cb, rows), F32),
        vmem((n, hr + SCALE_ROWS, cb), jnp.bfloat16),
        vmem((n, hr + SCALE_ROWS, cb), jnp.bfloat16),
        vmem((ny, max(nx - 1, 1), hr + SCALE_ROWS, cb), jnp.bfloat16),
        vmem((nx, max(ny - 1, 1), hr + SCALE_ROWS, cb), jnp.bfloat16),
        vmem((max(ny - 1, 1), hr + SCALE_ROWS, cb), jnp.bfloat16),
        vmem((max(nx - 1, 1), hr + SCALE_ROWS, cb), jnp.bfloat16),
        vmem((max(ny - 1, 1), hr + SCALE_ROWS, cb), jnp.bfloat16),
        vmem((max(nx - 1, 1), hr + SCALE_ROWS, cb), jnp.bfloat16),
        vmem((hr, cb), F32),
        vmem((hr, cb), F32),
        vmem((2, n, sr, k), F32),
        vmem((2, n - 1, sr, k), F32),
        vmem((2, n, sr, k), F32),
        vmem((2, n, sr, k), F32),
        vmem((2, n - 1, sr, k), F32),
        vmem((2, n, sr, k), F32),
        vmem((2, n, gr, k), F32),
        vmem((2, n - 1, gr, k), F32),
        vmem((2, n, gr, k), F32),
        vmem((k, 2 * k), F32),
        dma((4,)),
        dma((far, PARTS)), dma((far, PARTS)), dma((far, PARTS)), dma((far, PARTS)),
        dma((nz, PARTS)), dma((nz, PARTS)),
        dma((2,)), dma((2,)),
        dma((n,)), dma((ny, max(nx - 1, 1))),
        dma((n,)), dma((nx, max(ny - 1, 1))),
        dma((max(ny - 1, 1),)), dma((max(ny - 1, 1),)),
        dma((max(nx - 1, 1),)), dma((max(nx - 1, 1),)),
        dma((2,)), dma((2,)), dma((2,)), dma((2,)),
        dma((2,)), dma((2,)), dma((2,)), dma((2,)),
        dma((2,)), dma((2,)), dma((2,)), dma((2,)),
        dma((2, 4, max(nx, ny))), dma((2, 4, max(nx, ny))),
        dma((2, nx + ny)), dma((2, nx + ny)),
    ]
    any_space = pl.BlockSpec(memory_space=pl.ANY)
    in_vmem = pl.BlockSpec(memory_space=pltpu.VMEM)
    merged, lhat, s, sown, inverse, momentum = pl.pallas_call(
        functools.partial(body, nx, ny, nz, 1.0 / n),
        out_shape=(
            jax.ShapeDtypeStruct((rows, total), F32),
            jax.ShapeDtypeStruct((rows, k), F32),
            jax.ShapeDtypeStruct((nx, ny, 2, nz, sr, k), F32),
            jax.ShapeDtypeStruct((cb, k), F32),
            jax.ShapeDtypeStruct((k, k), F32),
            jax.ShapeDtypeStruct((rows, total), momentum.dtype),
        ),
        in_specs=[any_space] * 5,
        out_specs=(in_vmem,) * 6,
        scratch_shapes=scratch,
        compiler_params=pltpu.CompilerParams(
            collective_id=0, has_side_effects=True, vmem_limit_bytes=VMEM_LIMIT
        ),
        name="compress",
    )(*[pltpu.with_memory_space_constraint(v, pltpu.HBM) for v in (grad_out, activations, error_feedback, right_factor, momentum)])
    s = s.reshape(n, 2, nz, sr, k)
    wide = min(512, total)
    return pl.pallas_call(
        functools.partial(finish_body, wide),
        out_shape=(
            jax.ShapeDtypeStruct((1, rows, total), F32),
            jax.ShapeDtypeStruct((rows, total), jnp.bfloat16),
            jax.ShapeDtypeStruct((cb, k), F32),
        ),
        in_specs=[in_vmem] * 6,
        out_specs=(any_space, any_space, in_vmem),
        scratch_shapes=[
            vmem((total // wide, rows, wide), F32),
            vmem((total // wide, rows, wide), jnp.bfloat16),
            dma((total // wide, 2)),
        ],
        compiler_params=pltpu.CompilerParams(vmem_limit_bytes=20 << 20),
        name="finish",
    )(merged, lhat, s, momentum, sown, inverse)


def build(mesh, nx, ny, nz):
    return jax.shard_map(
        functools.partial(per_device, nx, ny, nz),
        mesh=mesh,
        in_specs=(
            P("dp", "rows"),
            P("dp", "rows"),
            P("dp", "rows", None),
            P("rows", None),
            P("rows", None),
        ),
        out_specs=(P("dp", "rows", None), P("rows", None), P("rows", None)),
        check_vma=False,
    )


def solution(mesh):
    return build(mesh, 4, 4, 8)
```
